128 devices in a mesh: lat: 8 (over z, core), lon: 16 (over x, y).
Axes of the slice: x: 4, y: 4, z: 4, core: 2. Of those that a mesh axis runs over, the one named last changes fastest.
Arguments:
- background: bfloat16 [131072, 384], P(('lat', 'lon')), may hold values from -6 to 6
- increment: bfloat16 [131072, 384], P(('lat', 'lon')), may hold values from -6 to 6
- coefficients: bfloat16 [384, 4352], replicated, may hold values from -0.3125 to 0.3125
- departures: bfloat16 [512, 128, 4352], P(('lat', 'lon')), may hold values from -24 to 24
- bias_pred: float32 [512, 128, 8], P(('lat', 'lon')), may hold values from -6 to 6
- beta_incr: float32 [8, 4352], replicated, may hold values from -2 to 2
- obs_weight: float32 [4352], replicated, may hold values from 0.1 to 1
- obs_count: int32 [512], P(('lat', 'lon')), may hold values from 1 to 128
- col_index: int32 [512, 128], P(('lat', 'lon')), may hold values from 0 to 131071, as said below
Outputs:
- radiance: bfloat16 [512, 128, 4352], P(('lat', 'lon'))
- column_grad: bfloat16 [131072, 384], P(('lat', 'lon'))
- bias_grad: float32 [4352, 8], P(('lat', 'lon'))
The draws below stay inside these ranges and needn't reach their ends.
Inputs may be any that keep to these rules, and one draw needn't show every extreme that they name: `col_index`: column c is owned by the block of 1024 columns c // 1024. Among the 512 slots of the blocks of one device, at most 6 name columns of any one owner, and some owner is named by exactly 6 slots of every device.
All inputs are finite; a program needn't handle non-finite values.
Results may differ from the reference program's by a relative error of at most 0.005.
Values may be sent and summed in bfloat16 or wider, within the bound.
No kernel may reach another device: no remote copies, remote signals or barrier semaphores. Data moves between devices by JAX's collectives and lax.ppermute only.
A program may use at most 128 MiB of HBM per device.

```python
import math
import jax
import jax.numpy as jnp
from jax import lax

P_SIZE = 384
CH = 4352
NPRED = 8
COLS_DEV = 1024
BLK = 128
NB_DEV = 4
NCOLS = 131072
NBLOCKS = 512
N_LAT = 8
N_LON = 16


def draw_col_index(key, part):
    devices = N_LAT * N_LON
    slot_count = NB_DEV * BLK
    quota = slot_count // (2 * devices)
    common_owner = jax.random.randint(jax.random.fold_in(key, 7), (), 0, devices).astype(jnp.int32)

    def one_device(device_index):
        device_key = jax.random.fold_in(key, device_index + 11)
        key_perm, key_order, key_local = jax.random.split(device_key, 3)
        others = (common_owner + 1 + jax.random.permutation(key_perm, devices - 1).astype(jnp.int32)) % devices
        hot_owners = jnp.concatenate([common_owner[None], others[:devices // 2 - 1]])
        spread_owners = jnp.arange(devices * quota, dtype=jnp.int32) // quota
        hot_extra = jnp.repeat(hot_owners, 2 * quota, total_repeat_length=devices * quota).astype(jnp.int32)
        owners = jnp.concatenate([spread_owners, hot_extra])
        owners = jax.random.permutation(key_order, owners).astype(jnp.int32)
        local_cols = jax.random.randint(key_local, (slot_count,), 0, COLS_DEV).astype(jnp.int32)
        return owners * COLS_DEV + local_cols
    columns = jax.vmap(one_device)(jnp.arange(devices, dtype=jnp.int32))
    return columns.reshape(NB_DEV * devices, BLK).astype(jnp.int32)


def touch_ends(result, own_key, low, largest):
    longest = result.shape.index(max(result.shape))
    spots = []
    for shift in (0, 1):
        where = [jax.random.randint(jax.random.fold_in(own_key, axis), (), 0, length) for axis, length in enumerate(result.shape)]
        where[longest] = (where[longest] + shift) % result.shape[longest]
        spots.append(tuple(where))
    return result.at[spots[0]].set(low).at[spots[1]].set(largest)


def spiked(drawn, stream_key, source, target, parts, factor):
    owner, partner = [(jnp.arange(drawn.shape[dim]) // (drawn.shape[dim] // parts)).reshape([-1 if axis == dim else 1 for axis in range(drawn.ndim)]) for dim in (source, target)]
    chosen = jax.random.permutation(stream_key, parts)[partner]
    strong = (owner == chosen) | (owner == (partner + parts // 2) % parts)
    return jnp.where(strong, factor * drawn, drawn)


def block_levels(stream_key, dims, shards, smallest, top_value):
    loudness, own = 1.0, jax.random.fold_in(stream_key, 6)
    for position, blocks in shards:
        heights = jnp.exp(jax.random.uniform(jax.random.fold_in(own, position), (blocks,), jnp.float32, smallest / len(shards), top_value / len(shards)))
        loudness = loudness * jnp.repeat(heights, dims[position] // blocks).reshape([-1 if axis == position else 1 for axis in range(len(dims))])
    return loudness


def bell_draw(rng, dims, width, bound, cuts=(), held_as=jnp.bfloat16):
    factor_of = block_levels(rng, dims, cuts, -0.22, 0.18) if cuts else 1.0
    values = jax.random.normal(rng, dims, jnp.float32) * width * factor_of
    return jnp.minimum(jnp.maximum(values, -bound), bound).astype(held_as)


def bell_draw_with(stream_key, dims, width, limit, shards, heavy, kind=jnp.bfloat16):
    drawn = width * jax.random.normal(stream_key, dims, jnp.float32)
    if shards:
        drawn = drawn * block_levels(stream_key, dims, shards, -0.22, 0.18)
    return jnp.clip(spiked(drawn, jax.random.fold_in(stream_key, 3), *heavy), -limit, limit).astype(kind)


def setup_inputs(seed: int = 0) -> dict:
    key_list = jax.random.split(jax.random.key(seed), 10)
    background = bell_draw(key_list[0], (NCOLS, P_SIZE), 1.0, 6.0, ((0, 128),))
    increment = bell_draw(key_list[1], (NCOLS, P_SIZE), 1.0, 6.0, ((0, 128),))
    coefficients = bell_draw(key_list[2], (P_SIZE, CH), P_SIZE ** -0.5, 0.3125)
    departures = bell_draw_with(key_list[3], (NBLOCKS, BLK, CH), 1.0, 24.0, ((0, 128),), (0, 2, 128, 5.5))
    bias_pred = bell_draw(key_list[4], (NBLOCKS, BLK, NPRED), 1.0, 6.0, ((0, 128),), jnp.float32)
    beta_incr = bell_draw(key_list[5], (NPRED, CH), NPRED ** -0.5, 2.0, (), jnp.float32)
    obs_weight = jnp.clip(jnp.exp(jax.random.uniform(key_list[6], (CH,), jnp.float32, math.log(0.1), math.log(1.0))), 0.1, 1.0)
    obs_count = touch_ends(jax.random.randint(key_list[7], (NBLOCKS,), 1, BLK + 1), jax.random.fold_in(key_list[7], 1), 1, BLK).astype(jnp.int32)
    col_index = draw_col_index(jax.random.fold_in(key_list[9], 71), 0)
    return {"background": background, "increment": increment, "coefficients": coefficients, "departures": departures, "bias_pred": bias_pred, "beta_incr": beta_incr, "obs_weight": obs_weight, "obs_count": obs_count, "col_index": col_index}


def reference(background, increment, coefficients, departures, bias_pred, beta_incr, obs_weight, obs_count, col_index):
    devices = N_LAT * N_LON
    slot_count = NB_DEV * BLK
    scaling = 1.0 / jnp.sqrt(jnp.float32(NBLOCKS * BLK))
    grouped_cols = col_index.reshape(devices, slot_count)
    grouped_deps = departures.reshape(devices, slot_count, CH)
    grouped_pred = bias_pred.reshape(devices, slot_count, NPRED)
    grouped_counts = obs_count.reshape(devices, NB_DEV)

    def accumulate(gradient, group):
        columns, misfits_in, predictors_in, counts = group
        slot_pos = jnp.arange(BLK, dtype=jnp.int32)
        present = (slot_pos[None, :] < counts[:, None]).reshape(slot_count, 1)
        base_rows = background[columns]
        step_rows = increment[columns]
        jacobian = 1.0 + 0.5 * jnp.tanh(base_rows.astype(jnp.float32))
        predictor = (step_rows.astype(jnp.float32) * jacobian).astype(jnp.bfloat16)
        radiance_f = jnp.dot(predictor, coefficients, preferred_element_type=jnp.float32)
        radiance_f = radiance_f + jnp.dot(predictors_in, beta_incr, precision=lax.Precision.HIGHEST)
        radiance_f = jnp.where(present, radiance_f, jnp.float32(0.0))
        misfit = jnp.where(present, obs_weight[None, :] * (radiance_f - misfits_in.astype(jnp.float32)), jnp.float32(0.0))
        pulled = jnp.dot(misfit.astype(jnp.bfloat16), coefficients.T, preferred_element_type=jnp.float32)
        gradient = gradient.at[columns].add(pulled * jacobian)
        bias_part = jnp.dot(misfit.T, predictors_in, precision=lax.Precision.HIGHEST) * scaling
        return (gradient, (radiance_f.astype(jnp.bfloat16), bias_part))
    start = jnp.zeros((NCOLS, P_SIZE), jnp.float32)
    gradient, (radiances, bias_parts) = lax.scan(accumulate, start, (grouped_cols, grouped_deps, grouped_pred, grouped_counts))
    return (radiances.reshape(NBLOCKS, BLK, CH), gradient.astype(jnp.bfloat16), lax.optimization_barrier(jnp.sum(bias_parts, axis=0)))
```

```python
import jax
import jax.numpy as jnp
from jax import lax
from jax.experimental import pallas as pl
from jax.experimental.pallas import tpu as pltpu
from jax.sharding import Mesh
from jax.sharding import PartitionSpec as P

AXES = ("lat_0", "lat_1", "lon_0", "lon_1")
ROWS = 8
LANES = 128
PRED_STRIDE = 48
TILE = 256
F32 = jnp.float32
BF16 = jnp.bfloat16
VMEM = pl.BlockSpec(memory_space=pltpu.VMEM)
SMEM = pl.BlockSpec(memory_space=pltpu.SMEM)
ANY = pl.BlockSpec(memory_space=pl.ANY)


def iota(shape, dim):
    return lax.broadcasted_iota(jnp.int32, shape, dim)


def one_hot(mask):
    return jnp.where(mask, 1.0, 0.0).astype(BF16)


def dot(a, b, dims=((1,), (0,))):
    return lax.dot_general(a, b, (dims, ((), ())), preferred_element_type=F32)


def split(x):
    high = x.astype(BF16)
    return high, (x - high.astype(F32)).astype(BF16)


def index_kernel(count_ref, col_ref, req_ref, pos_ref, *, shift):
    blocks, block_len = col_ref.shape
    slots = blocks * block_len
    devices = req_ref.shape[0]
    cols = col_ref[...]
    owners = lax.shift_right_logical(cols, shift)
    local = (cols & ((1 << shift) - 1)) + 1
    owner_rows = iota((devices, block_len), 0)
    table = [one_hot(owner_rows == owners[k : k + 1, :]) for k in range(blocks)]
    table = jnp.concatenate(table, axis=1)
    earlier = one_hot(iota((slots, slots), 0) < iota((slots, slots), 1))
    counts = dot(table, earlier)
    ranked = jnp.sum(table.astype(F32) * counts, axis=0, keepdims=True).astype(jnp.int32)
    rank_rows = iota((LANES, block_len), 0)
    lane = iota((1, block_len), 1)
    high, low = [], []
    for k in range(blocks):
        rank = ranked[:, k * block_len : (k + 1) * block_len]
        mine = rank_rows == rank
        value = local[k : k + 1, :]
        high.append(jnp.where(mine, lax.shift_right_logical(value, 5), 0).astype(F32))
        low.append(jnp.where(mine, value & 31, 0).astype(F32))
        position = owners[k : k + 1, :] * ROWS + rank
        pos_ref[k : k + 1, :] = jnp.where(lane < count_ref[k], position, -1)
    high = jnp.concatenate(high, axis=1).astype(BF16)
    low = jnp.concatenate(low, axis=1).astype(BF16)
    nt = ((1,), (1,))
    req_ref[...] = (dot(table, high, nt) * 32.0 + dot(table, low, nt)).astype(jnp.int32) - 1


def owner_kernel(ids_ref, base_ref, step_ref, out_ref, pick_ref):
    devices = ids_ref.shape[0]
    columns = base_ref.shape[0]
    jacobian = 1.0 + 0.5 * jnp.tanh(base_ref[...].astype(F32))
    formed = (step_ref[...].astype(F32) * jacobian).astype(BF16)
    by_row = ids_ref[...].astype(F32).T[0:ROWS, :].astype(jnp.int32)
    lane = iota((2 * ROWS, columns), 1)
    for k in range(0, devices, 2):
        pair = [jnp.broadcast_to(by_row[:, d : d + 1], (ROWS, columns)) for d in (k, k + 1)]
        pair = jnp.concatenate(pair, axis=0)
        pick_ref[k * ROWS : (k + 2) * ROWS, :] = one_hot(pair == lane)
    out_ref[...] = dot(pick_ref[...], formed).astype(BF16)


def main_kernel(
    arrived_ref,
    pos_ref,
    pred_ref,
    beta_ref,
    weight_ref,
    count_ref,
    coef_hbm,
    dep_hbm,
    rad_hbm,
    out_ref,
    coef,
    dep,
    rad,
    mis,
    left,
    beta,
    sums,
    turned,
    coef_sem,
    dep_sem,
    rad_sem,
):
    blocks, npred, block_len = pred_ref.shape
    slots, channels = dep.shape
    profile = coef.shape[0]
    rows = arrived_ref.shape[0]
    devices = rows // ROWS
    share = channels // devices
    steps = channels // TILE

    def part(t):
        return pl.ds(t * TILE, TILE)

    def coef_copy(t):
        return pltpu.make_async_copy(coef_hbm.at[:, part(t)], coef.at[:, part(t)], coef_sem.at[t])

    def dep_copy(t):
        return pltpu.make_async_copy(dep_hbm.at[:, part(t)], dep.at[:, part(t)], dep_sem.at[t])

    def rad_copy(t):
        return pltpu.make_async_copy(rad.at[:, part(t)], rad_hbm.at[:, part(t)], rad_sem.at[t])

    for t in range(steps):
        coef_copy(t).start()
        dep_copy(t).start()

    lane = iota((1, block_len), 1)
    stack = []
    for k in range(blocks):
        here = pl.ds(k * block_len, block_len)
        row = jnp.broadcast_to(pos_ref[k : k + 1, :].astype(F32), (block_len, block_len))
        column = row.T.astype(jnp.int32)
        wide = jnp.concatenate([column] * (rows // block_len), axis=1)
        select = one_hot(wide == iota((block_len, rows), 1))
        left[here, 0:profile] = dot(select, arrived_ref[...]).astype(BF16)
        predictors = jnp.where(lane < count_ref[k], pred_ref[k], 0.0)
        high, low = split(predictors)
        high, low = high.astype(F32), low.astype(F32)
        stack.append(jnp.concatenate([high, low], axis=0))
        zeros = jnp.zeros((LANES - 4 * npred, block_len), F32)
        tall = jnp.concatenate([high, high, low, low, zeros], axis=0)
        left[here, profile : profile + LANES] = tall.T.astype(BF16)
    stack = jnp.concatenate(stack, axis=1).astype(BF16)
    high, low = split(beta_ref[...])
    high, low = high.astype(F32), low.astype(F32)
    zeros = jnp.zeros((LANES - 4 * npred, channels), F32)
    beta[...] = jnp.concatenate([high, low, high, low, zeros], axis=0).astype(BF16)

    for t in range(steps):
        cut = slice(t * TILE, (t + 1) * TILE)
        coef_copy(t).wait()
        right = jnp.concatenate([coef[:, cut], beta[:, cut]], axis=0)
        radiance = dot(left[...], right)
        rad[:, cut] = radiance.astype(BF16)
        rad_copy(t).start()
        dep_copy(t).wait()
        misfit = weight_ref[:, cut] * (radiance - dep[:, cut].astype(F32))
        high, low = split(misfit)
        mis[:, cut] = high
        from_high = dot(stack, high)
        from_low = dot(stack, low)
        sums[:, cut] = (
            from_high[0:npred] + from_high[npred:] + from_low[0:npred] + from_low[npred:]
        )

    pulled = dot(mis[...], coef[...], ((1,), (1,))).astype(BF16)

    for d in range(devices):
        turned[d, :, 0:share] = sums[:, d * share : (d + 1) * share]
    bias = jnp.concatenate(
        [
            jnp.concatenate(
                [turned[:, p, 0:share], jnp.zeros((devices, PRED_STRIDE - share), F32)], axis=1
            )
            for p in range(npred)
        ],
        axis=1,
    )
    high, low = split(bias)

    payload = jnp.concatenate([pulled, high, low], axis=0)
    step = 256
    for k in range(0, rows, step):
        index = iota((step, block_len), 0) + k
        place = [one_hot(index == pos_ref[b : b + 1, :]) for b in range(blocks)]
        device = iota((step, devices), 1) * ROWS
        index = iota((step, devices), 0) + k
        place += [one_hot(index == device + (ROWS - 2)), one_hot(index == device + (ROWS - 1))]
        place = jnp.concatenate(place, axis=1)
        out_ref[k : k + step, :] = dot(place, payload).astype(BF16)

    for t in range(steps):
        rad_copy(t).wait()


def final_kernel(ids_ref, base_ref, back_ref, grad_ref, bias_ref, *, scaling):
    devices = ids_ref.shape[0]
    columns = base_ref.shape[0]
    rows = back_ref.shape[0]
    npred, share = bias_ref.shape
    by_row = ids_ref[...].astype(F32).T[0:ROWS, :].astype(jnp.int32) + 1
    halves = jnp.concatenate(
        [lax.shift_right_logical(by_row, 5).astype(F32), (by_row & 31).astype(F32)], axis=0
    ).astype(BF16)
    spread = one_hot(lax.shift_right_logical(iota((devices, rows), 1), 3) == iota((devices, rows), 0))
    both = dot(halves, spread)
    both = both[0:ROWS] * 32.0 + both[ROWS:]
    mine = (iota((ROWS, rows), 1) & (ROWS - 1)) == iota((ROWS, rows), 0)
    wanted = jnp.sum(jnp.where(mine, both, 0.0), axis=0, keepdims=True).astype(jnp.int32) - 1
    step = 256
    for k in range(0, columns, step):
        place = one_hot(iota((step, rows), 0) + k == wanted)
        jacobian = 1.0 + 0.5 * jnp.tanh(base_ref[k : k + step, :].astype(F32))
        grad_ref[k : k + step, :] = (dot(place, back_ref[...]) * jacobian).astype(BF16)
    last = one_hot((iota((ROWS, rows), 1) & (ROWS - 1)) >= ROWS - 2)
    total = dot(last, back_ref[...])[0:1, :] * scaling
    for p in range(npred):
        bias_ref[p : p + 1, :] = total[:, p * PRED_STRIDE : p * PRED_STRIDE + share]


def exchange(x):
    return lax.all_to_all(x, AXES, split_axis=0, concat_axis=0, tiled=True)


def shards(
    background,
    increment,
    coefficients,
    departures,
    bias_pred,
    beta_incr,
    obs_weight,
    obs_count,
    col_index,
):
    devices = lax.axis_size(AXES)
    columns, profile = background.shape
    blocks, block_len = col_index.shape
    channels = coefficients.shape[1]
    npred = bias_pred.shape[2]
    slots = blocks * block_len
    rows = devices * ROWS
    shift = columns.bit_length() - 1
    assert columns == 1 << shift and channels % (TILE * 1) == 0
    scaling = float((slots * devices) ** -0.5)
    limit = pltpu.CompilerParams(vmem_limit_bytes=48 * 2**20)

    requests, position = pl.pallas_call(
        lambda *refs: index_kernel(*refs, shift=shift),
        out_shape=(
            jax.ShapeDtypeStruct((devices, LANES), jnp.int32),
            jax.ShapeDtypeStruct((blocks, block_len), jnp.int32),
        ),
        in_specs=[SMEM, VMEM],
        out_specs=(VMEM, VMEM),
        name="index",
    )(obs_count, col_index)
    ids = exchange(requests.reshape(devices, 1, LANES)).reshape(devices, LANES)

    formed = pl.pallas_call(
        owner_kernel,
        out_shape=jax.ShapeDtypeStruct((rows, profile), BF16),
        in_specs=[VMEM] * 3,
        out_specs=VMEM,
        scratch_shapes=[pltpu.VMEM((rows, columns), BF16)],
        name="owner",
    )(ids, background, increment)
    arrived = exchange(formed.reshape(devices, ROWS, profile)).reshape(rows, profile)

    steps = channels // TILE
    radiance, outgoing = pl.pallas_call(
        main_kernel,
        out_shape=(
            jax.ShapeDtypeStruct((slots, channels), BF16),
            jax.ShapeDtypeStruct((rows, profile), BF16),
        ),
        in_specs=[VMEM] * 5 + [SMEM] + [ANY] * 2,
        out_specs=(ANY, VMEM),
        scratch_shapes=[
            pltpu.VMEM((profile, channels), BF16),
            pltpu.VMEM((slots, channels), BF16),
            pltpu.VMEM((slots, channels), BF16),
            pltpu.VMEM((slots, channels), BF16),
            pltpu.VMEM((slots, profile + LANES), BF16),
            pltpu.VMEM((LANES, channels), BF16),
            pltpu.VMEM((npred, channels), F32),
            pltpu.VMEM((devices, npred, LANES), F32),
            pltpu.SemaphoreType.DMA((steps,)),
            pltpu.SemaphoreType.DMA((steps,)),
            pltpu.SemaphoreType.DMA((steps,)),
        ],
        compiler_params=limit,
        name="main",
    )(
        arrived,
        position,
        jnp.transpose(bias_pred, (0, 2, 1)),
        beta_incr,
        obs_weight.reshape(1, channels),
        obs_count,
        coefficients,
        departures.reshape(slots, channels),
    )
    returned = exchange(outgoing.reshape(devices, ROWS, profile)).reshape(rows, profile)

    column_grad, bias_grad = pl.pallas_call(
        lambda *refs: final_kernel(*refs, scaling=scaling),
        out_shape=(
            jax.ShapeDtypeStruct((columns, profile), BF16),
            jax.ShapeDtypeStruct((npred, channels // devices), F32),
        ),
        in_specs=[VMEM] * 3,
        out_specs=(VMEM, VMEM),
        name="final",
    )(ids, background, returned)
    return (
        radiance.reshape(blocks, block_len, channels),
        column_grad,
        jnp.transpose(bias_grad, (1, 0)),
    )


def solution(mesh):
    finer = Mesh(mesh.devices.reshape(4, 2, 4, 4), AXES)
    in_specs = (
        P(AXES, None),
        P(AXES, None),
        P(),
        P(AXES, None, None),
        P(AXES, None, None),
        P(),
        P(),
        P(AXES),
        P(AXES, None),
    )
    out_specs = (P(AXES, None, None), P(AXES, None), P(AXES, None))
    return jax.shard_map(
        shards, mesh=finer, in_specs=in_specs, out_specs=out_specs, check_vma=False
    )
```

```python
import jax
import jax.numpy as jnp
from jax import lax
from jax.experimental import pallas as pl
from jax.experimental.pallas import tpu as pltpu
from jax.sharding import Mesh
from jax.sharding import PartitionSpec as P

AXES = ("lat_0", "lat_1", "lon_0", "lon_1")
ROWS = 8
LANES = 128
PRED_STRIDE = 48
TILE = 256
F32 = jnp.float32
BF16 = jnp.bfloat16
VMEM = pl.BlockSpec(memory_space=pltpu.VMEM)
SMEM = pl.BlockSpec(memory_space=pltpu.SMEM)
ANY = pl.BlockSpec(memory_space=pl.ANY)


def iota(shape, dim):
    return lax.broadcasted_iota(jnp.int32, shape, dim)


def one_hot(mask):
    return jnp.where(mask, 1.0, 0.0).astype(BF16)


def dot(a, b, dims=((1,), (0,))):
    return lax.dot_general(a, b, (dims, ((), ())), preferred_element_type=F32)


def split(x):
    high = x.astype(BF16)
    return high, (x - high.astype(F32)).astype(BF16)


def index_kernel(count_ref, col_ref, req_ref, pos_ref, *, shift):
    blocks, block_len = col_ref.shape
    slots = blocks * block_len
    devices = req_ref.shape[0]
    cols = col_ref[...]
    owners = lax.shift_right_logical(cols, shift)
    local = (cols & ((1 << shift) - 1)) + 1
    owner_rows = iota((devices, block_len), 0)
    table = [one_hot(owner_rows == owners[k : k + 1, :]) for k in range(blocks)]
    table = jnp.concatenate(table, axis=1)
    earlier = one_hot(iota((slots, slots), 0) < iota((slots, slots), 1))
    counts = dot(table, earlier)
    ranked = jnp.sum(table.astype(F32) * counts, axis=0, keepdims=True).astype(jnp.int32)
    rank_rows = iota((LANES, block_len), 0)
    lane = iota((1, block_len), 1)
    high, low = [], []
    for k in range(blocks):
        rank = ranked[:, k * block_len : (k + 1) * block_len]
        mine = rank_rows == rank
        value = local[k : k + 1, :]
        high.append(jnp.where(mine, lax.shift_right_logical(value, 5), 0).astype(F32))
        low.append(jnp.where(mine, value & 31, 0).astype(F32))
        position = owners[k : k + 1, :] * ROWS + rank
        pos_ref[k : k + 1, :] = jnp.where(lane < count_ref[k], position, -1)
    high = jnp.concatenate(high, axis=1).astype(BF16)
    low = jnp.concatenate(low, axis=1).astype(BF16)
    nt = ((1,), (1,))
    req_ref[...] = (dot(table, high, nt) * 32.0 + dot(table, low, nt)).astype(jnp.int32) - 1


def beta_rows(beta):
    high, low = split(beta)
    return jnp.concatenate([high.astype(F32), low.astype(F32)], axis=0).astype(BF16)


def form_kernel(base_ref, step_ref, form_ref):
    jacobian = 1.0 + 0.5 * jnp.tanh(base_ref[...].astype(F32))
    form_ref[...] = (step_ref[...].astype(F32) * jacobian).astype(BF16)


def second_kernel(
    pred_ref,
    count_ref,
    beta_ref,
    weight_ref,
    coef_hbm,
    dep_hbm,
    norm_ref,
    base_ref,
    sums_ref,
    side_ref,
    stack_ref,
    coef,
    dep,
    scaled,
    coef_sem,
    dep_sem,
):
    blocks, npred, block_len = pred_ref.shape
    profile, channels = coef.shape
    slots = dep.shape[0]
    pieces = coef_sem.shape[0]
    size = channels // pieces

    def coef_copy(t):
        cut = pl.ds(t * size, size)
        return pltpu.make_async_copy(coef_hbm.at[:, cut], coef.at[:, cut], coef_sem.at[t])

    def dep_copy(t):
        part = pl.ds(t * (slots // dep_sem.shape[0]), slots // dep_sem.shape[0])
        return pltpu.make_async_copy(dep_hbm.at[part], dep.at[part], dep_sem.at[t])

    for t in range(pieces):
        coef_copy(t).start()
    for t in range(dep_sem.shape[0]):
        dep_copy(t).start()

    lane = iota((1, block_len), 1)
    stack = []
    for k in range(blocks):
        predictors = jnp.where(lane < count_ref[k], pred_ref[k], 0.0)
        high, low = split(predictors)
        high, low = high.astype(F32), low.astype(F32)
        stack.append(jnp.concatenate([high, low], axis=0))
        zeros = jnp.zeros((LANES - 4 * npred, block_len), F32)
        tall = jnp.concatenate([high, high, low, low, zeros], axis=0)
        side_ref[k * block_len : (k + 1) * block_len, :] = tall.T.astype(BF16)
    stack = jnp.concatenate(stack, axis=1).astype(BF16)
    stack_ref[...] = stack
    for t in range(pieces):
        cut = slice(t * size, (t + 1) * size)
        coef_copy(t).wait()
        high, low = split(weight_ref[:, cut] * coef[:, cut].astype(F32))
        scaled[0:profile, cut] = high
        scaled[profile:, cut] = low
    for t in range(dep_sem.shape[0]):
        dep_copy(t).wait()
    nt = ((1,), (1,))
    pair = dot(dep[...], scaled[...], nt)
    base_ref[...] = pair[:, 0:profile] + pair[:, profile:]
    rows = jnp.concatenate([coef[...], beta_rows(beta_ref[...])], axis=0)
    pair = dot(rows, scaled[...], nt)
    high, low = split(pair[:, 0:profile] + pair[:, profile:])
    both = jnp.concatenate([high, low], axis=1)
    norm_ref[0 : profile + 2 * npred, :] = both
    norm_ref[profile + 2 * npred :, :] = both[profile:, :]
    sums = dot(stack, dep[...])
    sums_ref[...] = sums[0:npred] + sums[npred:]


def owner_kernel(ids_ref, form_ref, out_ref, pick_ref):
    devices = ids_ref.shape[0]
    columns = form_ref.shape[0]
    by_row = ids_ref[...].astype(F32).T[0:ROWS, :].astype(jnp.int32)
    lane = iota((2 * ROWS, columns), 1)
    for k in range(0, devices, 2):
        pair = [jnp.broadcast_to(by_row[:, d : d + 1], (ROWS, columns)) for d in (k, k + 1)]
        pair = jnp.concatenate(pair, axis=0)
        pick_ref[k * ROWS : (k + 2) * ROWS, :] = one_hot(pair == lane)
    out_ref[...] = dot(pick_ref[...], form_ref[...]).astype(BF16)


def main_kernel(
    arrived_ref,
    pos_ref,
    side_ref,
    stack_ref,
    norm_ref,
    base_ref,
    weight_ref,
    sums_ref,
    beta_ref,
    coef_hbm,
    out_ref,
    left_ref,
    sums,
    turned,
    coef,
    coef_sem,
):
    blocks, block_len = pos_ref.shape
    profile = arrived_ref.shape[1]
    rows = arrived_ref.shape[0]
    npred, channels = sums.shape
    devices = rows // ROWS
    share = channels // devices
    depth = norm_ref.shape[0]
    coef_copy = pltpu.make_async_copy(coef_hbm, coef, coef_sem)
    coef_copy.start()

    for k in range(blocks):
        here = pl.ds(k * block_len, block_len)
        row = jnp.broadcast_to(pos_ref[k : k + 1, :].astype(F32), (block_len, block_len))
        column = row.T.astype(jnp.int32)
        wide = jnp.concatenate([column] * (rows // block_len), axis=1)
        select = one_hot(wide == iota((block_len, rows), 1))
        left_ref[here, 0:profile] = dot(select, arrived_ref[...]).astype(BF16)
    left_ref[:, profile:] = side_ref[...]
    left = left_ref[:, 0:depth]

    pulled = dot(left, norm_ref[...])
    pulled = (pulled[:, 0:profile] + pulled[:, profile:] - base_ref[...]).astype(BF16)

    mixed = dot(stack_ref[...], left)
    high, low = split(mixed[0:npred] + mixed[npred:])
    mixed = jnp.concatenate([high.astype(F32), low.astype(F32)], axis=0).astype(BF16)
    tail = beta_rows(beta_ref[...])
    coef_copy.wait()
    mixed = dot(mixed, jnp.concatenate([coef[...], tail, tail], axis=0))
    sums[...] = weight_ref[...] * (mixed[0:npred] + mixed[npred:] - sums_ref[...])
    for d in range(devices):
        turned[d, :, 0:share] = sums[:, d * share : (d + 1) * share]
    bias = jnp.concatenate(
        [
            jnp.concatenate(
                [turned[:, p, 0:share], jnp.zeros((devices, PRED_STRIDE - share), F32)], axis=1
            )
            for p in range(npred)
        ],
        axis=1,
    )
    high, low = split(bias)
    payload = jnp.concatenate([pulled, high, low], axis=0)
    step = 256
    for k in range(0, rows, step):
        index = iota((step, block_len), 0) + k
        place = [one_hot(index == pos_ref[b : b + 1, :]) for b in range(blocks)]
        device = iota((step, devices), 1) * ROWS
        index = iota((step, devices), 0) + k
        place += [one_hot(index == device + (ROWS - 2)), one_hot(index == device + (ROWS - 1))]
        place = jnp.concatenate(place, axis=1)
        out_ref[k : k + step, :] = dot(place, payload).astype(BF16)


def radiance_kernel(left_ref, beta_ref, coef_hbm, out_hbm, out, coef, sem, coef_sem):
    profile, channels = coef.shape
    npred = beta_ref.shape[0]
    depth = profile + 4 * npred
    steps = channels // TILE

    def copy(t):
        cut = pl.ds(t * TILE, TILE)
        return pltpu.make_async_copy(out.at[:, cut], out_hbm.at[:, cut], sem.at[t])

    def coef_copy(t):
        cut = pl.ds(t * TILE, TILE)
        return pltpu.make_async_copy(coef_hbm.at[:, cut], coef.at[:, cut], coef_sem.at[t])

    for t in range(steps):
        coef_copy(t).start()
    tail = beta_rows(beta_ref[...])
    for t in range(steps):
        cut = slice(t * TILE, (t + 1) * TILE)
        coef_copy(t).wait()
        right = jnp.concatenate([coef[:, cut], tail[:, cut], tail[:, cut]], axis=0)
        out[:, cut] = dot(left_ref[:, 0:depth], right).astype(BF16)
        copy(t).start()
    for t in range(steps):
        copy(t).wait()


def final_kernel(ids_ref, base_ref, back_ref, grad_ref, bias_ref, *, scaling):
    devices = ids_ref.shape[0]
    columns = base_ref.shape[0]
    rows = back_ref.shape[0]
    npred, share = bias_ref.shape
    by_row = ids_ref[...].astype(F32).T[0:ROWS, :].astype(jnp.int32) + 1
    halves = jnp.concatenate(
        [lax.shift_right_logical(by_row, 5).astype(F32), (by_row & 31).astype(F32)], axis=0
    ).astype(BF16)
    spread = one_hot(lax.shift_right_logical(iota((devices, rows), 1), 3) == iota((devices, rows), 0))
    both = dot(halves, spread)
    both = both[0:ROWS] * 32.0 + both[ROWS:]
    mine = (iota((ROWS, rows), 1) & (ROWS - 1)) == iota((ROWS, rows), 0)
    wanted = jnp.sum(jnp.where(mine, both, 0.0), axis=0, keepdims=True).astype(jnp.int32) - 1
    step = 256
    for k in range(0, columns, step):
        place = one_hot(iota((step, rows), 0) + k == wanted)
        jacobian = 1.0 + 0.5 * jnp.tanh(base_ref[k : k + step, :].astype(F32))
        grad_ref[k : k + step, :] = (dot(place, back_ref[...]) * jacobian).astype(BF16)
    last = one_hot((iota((ROWS, rows), 1) & (ROWS - 1)) >= ROWS - 2)
    total = dot(last, back_ref[...])[0:1, :] * scaling
    for p in range(npred):
        bias_ref[p : p + 1, :] = total[:, p * PRED_STRIDE : p * PRED_STRIDE + share]


def exchange(x):
    return lax.all_to_all(x, AXES, split_axis=0, concat_axis=0, tiled=True)


def shards(
    background,
    increment,
    coefficients,
    departures,
    bias_pred,
    beta_incr,
    obs_weight,
    obs_count,
    col_index,
):
    devices = lax.axis_size(AXES)
    columns, profile = background.shape
    blocks, block_len = col_index.shape
    channels = coefficients.shape[1]
    npred = bias_pred.shape[2]
    slots = blocks * block_len
    rows = devices * ROWS
    shift = columns.bit_length() - 1
    assert columns == 1 << shift and channels % (TILE * 1) == 0
    scaling = float((slots * devices) ** -0.5)
    depth = profile + 4 * npred

    def shape(*dims, dtype=BF16):
        return jax.ShapeDtypeStruct(dims, dtype)

    def call(kernel, outs, inputs, flops, in_specs=None, out_specs=None, scratch=(), vmem=None):
        return pl.pallas_call(
            kernel,
            out_shape=outs,
            in_specs=in_specs or [VMEM] * len(inputs),
            out_specs=out_specs or jax.tree.map(lambda _: VMEM, outs),
            scratch_shapes=scratch,
            compiler_params=pltpu.CompilerParams(vmem_limit_bytes=vmem and vmem * 2**20),
            cost_estimate=pl.CostEstimate(
                flops=int(flops), bytes_accessed=4 * 2**20, transcendentals=0
            ),
        )(*inputs)

    flat_dep = pltpu.with_memory_space_constraint(departures.reshape(slots, channels), pltpu.HBM)
    coef_hbm = pltpu.with_memory_space_constraint(coefficients, pltpu.HBM)
    weight = obs_weight.reshape(1, channels)
    requests, position = call(
        lambda *refs: index_kernel(*refs, shift=shift),
        (shape(devices, LANES, dtype=jnp.int32), shape(blocks, block_len, dtype=jnp.int32)),
        (obs_count, col_index),
        1e8,
        in_specs=[SMEM, VMEM],
    )
    ids = exchange(requests.reshape(devices, 1, LANES)).reshape(devices, LANES)
    formed = call(form_kernel, shape(columns, profile), (background, increment), 3e9, vmem=16)
    rows_out = call(
        owner_kernel,
        shape(rows, profile),
        (ids, formed),
        1e9,
        scratch=[pltpu.VMEM((rows, columns), BF16)],
        vmem=16,
    )
    arrived = exchange(rows_out.reshape(devices, ROWS, profile)).reshape(rows, profile)
    norm, base, base_sums, side, stack = call(
        second_kernel,
        (
            shape(depth, 2 * profile),
            shape(slots, profile, dtype=F32),
            shape(npred, channels, dtype=F32),
            shape(slots, LANES),
            shape(2 * npred, slots),
        ),
        (jnp.transpose(bias_pred, (0, 2, 1)), obs_count, beta_incr, weight, coef_hbm, flat_dep),
        8e9,
        in_specs=[VMEM, SMEM, VMEM, VMEM, ANY, ANY],
        scratch=[
            pltpu.VMEM((profile, channels), BF16),
            pltpu.VMEM((slots, channels), BF16),
            pltpu.VMEM((2 * profile, channels), BF16),
            pltpu.SemaphoreType.DMA((channels // TILE,)),
            pltpu.SemaphoreType.DMA((4,)),
        ],
        vmem=32,
    )
    outgoing, left = call(
        main_kernel,
        (shape(rows, profile), shape(slots, profile + LANES)),
        (arrived, position, side, stack, norm, base, weight, base_sums, beta_incr, coef_hbm),
        2e9,
        in_specs=[VMEM] * 9 + [ANY],
        scratch=[
            pltpu.VMEM((npred, channels), F32),
            pltpu.VMEM((devices, npred, LANES), F32),
            pltpu.VMEM((profile, channels), BF16),
            pltpu.SemaphoreType.DMA,
        ],
        vmem=24,
    )
    returned = exchange(outgoing.reshape(devices, ROWS, profile)).reshape(rows, profile)
    radiance = call(
        radiance_kernel,
        shape(slots, channels),
        (left, beta_incr, coef_hbm),
        3e9,
        in_specs=[VMEM, VMEM, ANY],
        out_specs=ANY,
        scratch=[
            pltpu.VMEM((slots, channels), BF16),
            pltpu.VMEM((profile, channels), BF16),
            pltpu.SemaphoreType.DMA((channels // TILE,)),
            pltpu.SemaphoreType.DMA((channels // TILE,)),
        ],
        vmem=32,
    )
    column_grad, bias_grad = call(
        lambda *refs: final_kernel(*refs, scaling=scaling),
        (shape(columns, profile), shape(npred, channels // devices, dtype=F32)),
        (ids, background, returned),
        1e9,
        vmem=16,
    )
    return (
        radiance.reshape(blocks, block_len, channels),
        column_grad,
        jnp.transpose(bias_grad, (1, 0)),
    )


def solution(mesh):
    finer = Mesh(mesh.devices.reshape(4, 2, 4, 4), AXES)
    in_specs = (
        P(AXES, None),
        P(AXES, None),
        P(),
        P(AXES, None, None),
        P(AXES, None, None),
        P(),
        P(),
        P(AXES),
        P(AXES, None),
    )
    out_specs = (P(AXES, None, None), P(AXES, None), P(AXES, None))
    return jax.shard_map(
        shards, mesh=finer, in_specs=in_specs, out_specs=out_specs, check_vma=False
    )
```

```python
import jax
import jax.numpy as jnp
from jax import lax
from jax.experimental import pallas as pl
from jax.experimental.pallas import tpu as pltpu
from jax.sharding import Mesh
from jax.sharding import PartitionSpec as P

AXES = ("lat_0", "lat_1", "lon_0", "lon_1")
RANKS = 6
ROWS = 8
LANES = 128
PRED_STRIDE = 48
TILE = 256
F32 = jnp.float32
BF16 = jnp.bfloat16
VMEM = pl.BlockSpec(memory_space=pltpu.VMEM)
SMEM = pl.BlockSpec(memory_space=pltpu.SMEM)
ANY = pl.BlockSpec(memory_space=pl.ANY)


def iota(shape, dim):
    return lax.broadcasted_iota(jnp.int32, shape, dim)


def one_hot(mask):
    return jnp.where(mask, 1.0, 0.0).astype(BF16)


def dot(a, b, dims=((1,), (0,))):
    return lax.dot_general(a, b, (dims, ((), ())), preferred_element_type=F32)


def split(x):
    high = x.astype(BF16)
    return high, (x - high.astype(F32)).astype(BF16)


def index_kernel(
    col_hbm, base_hbm, step_hbm, req_ref, pos_ref, form_ref, col_ref, base_ref, step_ref, sem, *, shift
):
    copies = [
        pltpu.make_async_copy(source, target, sem.at[k])
        for k, (source, target) in enumerate(
            [(col_hbm, col_ref), (base_hbm, base_ref), (step_hbm, step_ref)]
        )
    ]
    for copy in copies:
        copy.start()
    copies[0].wait()
    blocks, block_len = col_ref.shape
    slots = blocks * block_len
    devices = req_ref.shape[0]
    cols = col_ref[...]
    owners = lax.shift_right_logical(cols, shift)
    local = (cols & ((1 << shift) - 1)) + 1
    owner_rows = iota((devices, block_len), 0)
    table = [one_hot(owner_rows == owners[k : k + 1, :]) for k in range(blocks)]
    table = jnp.concatenate(table, axis=1)
    earlier = one_hot(iota((slots, slots), 0) < iota((slots, slots), 1))
    counts = dot(table, earlier)
    ranked = jnp.sum(table.astype(F32) * counts, axis=0, keepdims=True).astype(jnp.int32)
    rank_rows = iota((LANES, block_len), 0)
    high, low = [], []
    for k in range(blocks):
        rank = ranked[:, k * block_len : (k + 1) * block_len]
        mine = rank_rows == rank
        value = local[k : k + 1, :]
        high.append(jnp.where(mine, lax.shift_right_logical(value, 5), 0).astype(F32))
        low.append(jnp.where(mine, value & 31, 0).astype(F32))
        pos_ref[k : k + 1, :] = owners[k : k + 1, :] * ROWS + rank
    high = jnp.concatenate(high, axis=1).astype(BF16)
    low = jnp.concatenate(low, axis=1).astype(BF16)
    nt = ((1,), (1,))
    req_ref[...] = (dot(table, high, nt) * 32.0 + dot(table, low, nt)).astype(jnp.int32) - 1
    copies[1].wait()
    copies[2].wait()
    jacobian = 1.0 + 0.5 * jnp.tanh(base_ref[...].astype(F32))
    form_ref[...] = (step_ref[...].astype(F32) * jacobian).astype(BF16)


def beta_rows(beta):
    high, low = split(beta)
    return jnp.concatenate([high.astype(F32), low.astype(F32)], axis=0).astype(BF16)


def second_kernel(
    after_ref,
    pos_ref,
    pred_ref,
    count_ref,
    beta_ref,
    weight_ref,
    coef_hbm,
    dep_hbm,
    slot_ref,
    norm_ref,
    base_ref,
    sums_ref,
    side_ref,
    stack_ref,
    coef,
    dep,
    scaled,
    coef_sem,
    dep_sem,
):
    blocks, npred, block_len = pred_ref.shape
    profile, _ = coef.shape
    slots = dep.shape[0]
    pieces = coef_sem.shape[0]
    size = profile // pieces

    def coef_copy(t):
        cut = pl.ds(t * size, size)
        return pltpu.make_async_copy(coef_hbm.at[cut], coef.at[cut], coef_sem.at[t])

    def dep_copy(t):
        part = pl.ds(t * (slots // dep_sem.shape[0]), slots // dep_sem.shape[0])
        return pltpu.make_async_copy(dep_hbm.at[part], dep.at[part], dep_sem.at[t])

    for t in range(pieces):
        coef_copy(t).start()
    for t in range(dep_sem.shape[0]):
        dep_copy(t).start()

    lane = iota((1, block_len), 1)
    stack = []
    for k in range(blocks):
        slot_ref[k : k + 1, :] = jnp.where(lane < count_ref[k], pos_ref[k : k + 1, :], -1)
        predictors = jnp.where(lane < count_ref[k], pred_ref[k], 0.0)
        high, low = split(predictors)
        high, low = high.astype(F32), low.astype(F32)
        stack.append(jnp.concatenate([high, low], axis=0))
        zeros = jnp.zeros((LANES - 4 * npred, block_len), F32)
        tall = jnp.concatenate([high, high, low, low, zeros], axis=0)
        side_ref[k * block_len : (k + 1) * block_len, :] = tall.T.astype(BF16)
    stack = jnp.concatenate(stack, axis=1).astype(BF16)
    stack_ref[...] = stack
    for t in range(pieces):
        coef_copy(t).wait()
        cut = slice(t * size, (t + 1) * size)
        scaled[cut, :] = (weight_ref[...] * coef[cut, :].astype(F32)).astype(BF16)
    nt = ((1,), (1,))
    rows = jnp.concatenate([coef[...], beta_rows(beta_ref[...])], axis=0)
    both = jnp.concatenate(split(dot(rows, scaled[...], nt)), axis=1)
    norm_ref[0 : profile + 2 * npred, :] = both
    norm_ref[profile + 2 * npred :, :] = both[profile:, :]
    for t in range(dep_sem.shape[0]):
        dep_copy(t).wait()
    base_ref[...] = dot(dep[...], scaled[...], nt)
    sums = dot(stack, dep[...])
    sums_ref[...] = sums[0:npred] + sums[npred:]


def owner_kernel(ids_ref, form_ref, out_hbm, pick, wide, out, sem):
    devices = ids_ref.shape[0]
    columns, profile = form_ref.shape
    cuts = profile // LANES
    group = RANKS * cuts
    lane = iota((devices, columns), 1)
    for r in range(RANKS):
        pick[r * devices : (r + 1) * devices, :] = one_hot(ids_ref[:, r : r + 1] == lane)
    result = dot(pick[...], form_ref[...])
    for r in range(RANKS):
        for c in range(cuts):
            wide[pl.ds(c * RANKS + r, devices, stride=group), :] = result[
                r * devices : (r + 1) * devices, c * LANES : (c + 1) * LANES
            ]
    out[...] = wide[...].astype(BF16)
    copy = pltpu.make_async_copy(out, out_hbm, sem)
    copy.start()
    copy.wait()


def main_kernel(
    arrived_ref,
    pos_ref,
    side_ref,
    stack_ref,
    norm_ref,
    base_ref,
    weight_ref,
    sums_ref,
    beta_ref,
    coef_hbm,
    out_hbm,
    left_ref,
    sums,
    turned,
    placed,
    coef,
    out,
    table,
    chosen,
    coef_sem,
    out_sem,
):
    blocks, block_len = pos_ref.shape
    rows, profile = out.shape
    npred, channels = sums.shape
    devices = rows // ROWS
    cuts = profile // LANES
    share = channels // devices
    depth = norm_ref.shape[0]
    coef_copy = pltpu.make_async_copy(coef_hbm, coef, coef_sem)
    coef_copy.start()

    count = devices * RANKS
    group = RANKS * cuts
    batch = 8
    for g in range(devices // batch):
        rows_in = arrived_ref[g * batch * group : (g + 1) * batch * group, :]
        for c in range(cuts):
            first = [d * group + c * RANKS for d in range(batch)]
            part = jnp.concatenate([rows_in[f : f + RANKS, :] for f in first], axis=0)
            here = slice(g * batch * RANKS, (g + 1) * batch * RANKS)
            table[here, c * LANES : (c + 1) * LANES] = part
    for k in range(blocks):
        here = pl.ds(k * block_len, block_len)
        row = pos_ref[k : k + 1, :]
        owner = lax.shift_right_arithmetic(row, ROWS.bit_length() - 1)
        row = jnp.where(row < 0, -1, row - owner * (ROWS - RANKS))
        column = jnp.broadcast_to(row.astype(F32), (block_len, block_len)).T.astype(jnp.int32)
        lane = iota((block_len, count), 1)
        chosen[here, :] = one_hot(jnp.concatenate([column] * (count // block_len), axis=1) == lane)
    left_ref[:, 0:profile] = dot(chosen[...], table[...]).astype(BF16)
    left_ref[:, profile:] = side_ref[...]
    left = left_ref[:, 0:depth]

    pulled = dot(left, norm_ref[...])
    pulled = (pulled[:, 0:profile] + pulled[:, profile:] - base_ref[...]).astype(BF16)
    step = rows // out_sem.shape[0]

    def copy(t):
        cut = pl.ds(t * step, step)
        return pltpu.make_async_copy(out.at[cut], out_hbm.at[cut], out_sem.at[t])

    for k in range(0, rows, step):
        index = iota((step, block_len), 0) + k
        place = [one_hot(index == pos_ref[b : b + 1, :]) for b in range(blocks)]
        placed[k : k + step, :] = dot(jnp.concatenate(place, axis=1), pulled)

    mixed = dot(stack_ref[...], left)
    high, low = split(mixed[0:npred] + mixed[npred:])
    mixed = jnp.concatenate([high.astype(F32), low.astype(F32)], axis=0).astype(BF16)
    tail = beta_rows(beta_ref[...])
    coef_copy.wait()
    mixed = dot(mixed, jnp.concatenate([coef[...], tail, tail], axis=0))
    sums[...] = weight_ref[...] * (mixed[0:npred] + mixed[npred:] - sums_ref[...])
    for d in range(devices):
        turned[d, :, 0:share] = sums[:, d * share : (d + 1) * share]
    bias = jnp.concatenate(
        [
            jnp.concatenate(
                [turned[:, p, 0:share], jnp.zeros((devices, PRED_STRIDE - share), F32)], axis=1
            )
            for p in range(npred)
        ],
        axis=1,
    )
    bias = jnp.concatenate(split(bias), axis=0)
    for k in range(0, rows, step):
        device = iota((step, devices), 1) * ROWS
        index = iota((step, devices), 0) + k
        place = [one_hot(index == device + (ROWS - 2)), one_hot(index == device + (ROWS - 1))]
        extra = dot(jnp.concatenate(place, axis=1), bias)
        out[k : k + step, :] = (placed[k : k + step, :] + extra).astype(BF16)
        copy(k // step).start()
    for k in range(rows // step):
        copy(k).wait()


def radiance_kernel(left_ref, beta_ref, coef_hbm, out_hbm, out, coef, sem, coef_sem):
    profile, channels = coef.shape
    npred = beta_ref.shape[0]
    depth = profile + 4 * npred
    steps = channels // TILE

    def copy(t):
        cut = pl.ds(t * TILE, TILE)
        return pltpu.make_async_copy(out.at[:, cut], out_hbm.at[:, cut], sem.at[t])

    coef_copy = pltpu.make_async_copy(coef_hbm, coef, coef_sem)
    coef_copy.start()
    tail = beta_rows(beta_ref[...])
    coef_copy.wait()
    for t in range(steps):
        cut = slice(t * TILE, (t + 1) * TILE)
        right = jnp.concatenate([coef[:, cut], tail[:, cut], tail[:, cut]], axis=0)
        out[:, cut] = dot(left_ref[:, 0:depth], right).astype(BF16)
        copy(t).start()
    for t in range(steps):
        copy(t).wait()


def final_kernel(ids_ref, base_ref, back_ref, grad_ref, bias_ref, *, scaling):
    devices = ids_ref.shape[0]
    columns = base_ref.shape[0]
    rows = back_ref.shape[0]
    npred, share = bias_ref.shape
    by_row = ids_ref[...].astype(F32).T[0:ROWS, :].astype(jnp.int32) + 1
    halves = jnp.concatenate(
        [lax.shift_right_logical(by_row, 5).astype(F32), (by_row & 31).astype(F32)], axis=0
    ).astype(BF16)
    spread = one_hot(lax.shift_right_logical(iota((devices, rows), 1), 3) == iota((devices, rows), 0))
    both = dot(halves, spread)
    both = both[0:ROWS] * 32.0 + both[ROWS:]
    mine = (iota((ROWS, rows), 1) & (ROWS - 1)) == iota((ROWS, rows), 0)
    wanted = jnp.sum(jnp.where(mine, both, 0.0), axis=0, keepdims=True).astype(jnp.int32) - 1
    step = 256
    for k in range(0, columns, step):
        place = one_hot(iota((step, rows), 0) + k == wanted)
        jacobian = 1.0 + 0.5 * jnp.tanh(base_ref[k : k + step, :].astype(F32))
        grad_ref[k : k + step, :] = (dot(place, back_ref[...]) * jacobian).astype(BF16)
    last = one_hot((iota((ROWS, rows), 1) & (ROWS - 1)) >= ROWS - 2)
    total = dot(last, back_ref[...])[0:1, :] * scaling
    for p in range(npred):
        bias_ref[p : p + 1, :] = total[:, p * PRED_STRIDE : p * PRED_STRIDE + share]


def exchange(x):
    return lax.all_to_all(x, AXES, split_axis=0, concat_axis=0, tiled=True)


def shards(
    background,
    increment,
    coefficients,
    departures,
    bias_pred,
    beta_incr,
    obs_weight,
    obs_count,
    col_index,
):
    devices = lax.axis_size(AXES)
    columns, profile = background.shape
    blocks, block_len = col_index.shape
    channels = coefficients.shape[1]
    npred = bias_pred.shape[2]
    slots = blocks * block_len
    rows = devices * ROWS
    shift = columns.bit_length() - 1
    assert columns == 1 << shift and channels % (TILE * 1) == 0
    scaling = float((slots * devices) ** -0.5)
    depth = profile + 4 * npred
    group = RANKS * profile // LANES

    def shape(*dims, dtype=BF16):
        return jax.ShapeDtypeStruct(dims, dtype)

    def call(kernel, outs, inputs, flops, in_specs=None, out_specs=None, scratch=(), vmem=None):
        return pl.pallas_call(
            kernel,
            out_shape=outs,
            in_specs=in_specs or [VMEM] * len(inputs),
            out_specs=out_specs or ([VMEM] * len(outs) if isinstance(outs, tuple) else VMEM),
            scratch_shapes=scratch,
            compiler_params=pltpu.CompilerParams(vmem_limit_bytes=vmem and vmem * 2**20),
            cost_estimate=pl.CostEstimate(
                flops=int(flops), bytes_accessed=4 * 2**20, transcendentals=0
            ),
        )(*inputs)

    def in_hbm(x):
        return pltpu.with_memory_space_constraint(x, pltpu.HBM)

    flat_dep = in_hbm(departures.reshape(slots, channels))
    coef_hbm = in_hbm(coefficients)
    requests, position, formed = call(
        lambda *refs: index_kernel(*refs, shift=shift),
        (
            shape(devices, LANES, dtype=jnp.int32),
            shape(blocks, block_len, dtype=jnp.int32),
            shape(columns, profile),
        ),
        (in_hbm(col_index), in_hbm(background), in_hbm(increment)),
        1e8,
        in_specs=[ANY] * 3,
        scratch=[
            pltpu.VMEM((blocks, block_len), jnp.int32),
            pltpu.VMEM((columns, profile), BF16),
            pltpu.VMEM((columns, profile), BF16),
            pltpu.SemaphoreType.DMA((3,)),
        ],
        vmem=16,
    )
    ids = exchange(requests.reshape(devices, 1, LANES)).reshape(devices, LANES)
    ids, obs_weight = lax.optimization_barrier((ids, obs_weight))
    weight = obs_weight.reshape(1, channels)
    rows_out = call(
        owner_kernel,
        shape(devices * group, LANES),
        (ids, formed),
        1e9,
        out_specs=ANY,
        scratch=[
            pltpu.VMEM((devices * RANKS, columns), BF16),
            pltpu.VMEM((devices * group, LANES), F32),
            pltpu.VMEM((devices * group, LANES), BF16),
            pltpu.SemaphoreType.DMA,
        ],
        vmem=16,
    )
    arrived = exchange(rows_out.reshape(devices, group // 2, 2, LANES))
    arrived = arrived.reshape(devices * group, LANES)
    slot_pos, norm, base, base_sums, side, stack = call(
        second_kernel,
        (
            shape(blocks, block_len, dtype=jnp.int32),
            shape(depth, 2 * profile),
            shape(slots, profile, dtype=F32),
            shape(npred, channels, dtype=F32),
            shape(slots, LANES),
            shape(2 * npred, slots),
        ),
        (
            ids,
            position,
            jnp.transpose(bias_pred, (0, 2, 1)),
            obs_count,
            beta_incr,
            weight,
            coef_hbm,
            flat_dep,
        ),
        8e9,
        in_specs=[ANY, VMEM, VMEM, SMEM, VMEM, VMEM, ANY, ANY],
        scratch=[
            pltpu.VMEM((profile, channels), BF16),
            pltpu.VMEM((slots, channels), BF16),
            pltpu.VMEM((profile, channels), BF16),
            pltpu.SemaphoreType.DMA((4,)),
            pltpu.SemaphoreType.DMA((4,)),
        ],
        vmem=32,
    )
    outgoing, left = call(
        main_kernel,
        (shape(rows, profile), shape(slots, profile + LANES)),
        (arrived, slot_pos, side, stack, norm, base, weight, base_sums, beta_incr, coef_hbm),
        2e9,
        in_specs=[VMEM] * 9 + [ANY],
        out_specs=(ANY, VMEM),
        scratch=[
            pltpu.VMEM((npred, channels), F32),
            pltpu.VMEM((devices, npred, LANES), F32),
            pltpu.VMEM((rows, profile), F32),
            pltpu.VMEM((profile, channels), BF16),
            pltpu.VMEM((rows, profile), BF16),
            pltpu.VMEM((devices * RANKS, profile), BF16),
            pltpu.VMEM((slots, devices * RANKS), BF16),
            pltpu.SemaphoreType.DMA,
            pltpu.SemaphoreType.DMA((4,)),
        ],
        vmem=24,
    )
    returned = exchange(outgoing.reshape(devices, ROWS, profile)).reshape(rows, profile)
    radiance = call(
        radiance_kernel,
        shape(slots, channels),
        (left, beta_incr, coef_hbm),
        3e9,
        in_specs=[VMEM, VMEM, ANY],
        out_specs=ANY,
        scratch=[
            pltpu.VMEM((slots, channels), BF16),
            pltpu.VMEM((profile, channels), BF16),
            pltpu.SemaphoreType.DMA((channels // TILE,)),
            pltpu.SemaphoreType.DMA,
        ],
        vmem=32,
    )
    column_grad, bias_grad = call(
        lambda *refs: final_kernel(*refs, scaling=scaling),
        (shape(columns, profile), shape(npred, channels // devices, dtype=F32)),
        (ids, background, returned),
        1e9,
        vmem=16,
    )
    return (
        radiance.reshape(blocks, block_len, channels),
        column_grad,
        jnp.transpose(bias_grad, (1, 0)),
    )


def solution(mesh):
    finer = Mesh(mesh.devices.reshape(4, 2, 4, 4), AXES)
    in_specs = (
        P(AXES, None),
        P(AXES, None),
        P(),
        P(AXES, None, None),
        P(AXES, None, None),
        P(),
        P(),
        P(AXES),
        P(AXES, None),
    )
    out_specs = (P(AXES, None, None), P(AXES, None), P(AXES, None))
    return jax.shard_map(
        shards, mesh=finer, in_specs=in_specs, out_specs=out_specs, check_vma=False
    )
```

```python
import jax
import jax.numpy as jnp
from jax import lax
from jax.experimental import pallas as pl
from jax.experimental.pallas import tpu as pltpu
from jax.sharding import Mesh
from jax.sharding import PartitionSpec as P

AXES = ("lat_0", "lat_1", "lon_0", "lon_1")
RANKS = 6
ROWS = 8
LANES = 128
PRED_STRIDE = 48
TILE = 256
F32 = jnp.float32
BF16 = jnp.bfloat16
VMEM = pl.BlockSpec(memory_space=pltpu.VMEM)
SMEM = pl.BlockSpec(memory_space=pltpu.SMEM)
ANY = pl.BlockSpec(memory_space=pl.ANY)


def iota(shape, dim):
    return lax.broadcasted_iota(jnp.int32, shape, dim)


def one_hot(mask):
    return jnp.where(mask, 1.0, 0.0).astype(BF16)


def dot(a, b, dims=((1,), (0,))):
    return lax.dot_general(a, b, (dims, ((), ())), preferred_element_type=F32)


def split(x):
    high = x.astype(BF16)
    return high, (x - high.astype(F32)).astype(BF16)


def index_kernel(
    col_hbm, base_hbm, step_hbm, req_ref, pos_ref, form_ref, col_ref, base_ref, step_ref, sem, *, shift
):
    copies = [
        pltpu.make_async_copy(source, target, sem.at[k])
        for k, (source, target) in enumerate(
            [(col_hbm, col_ref), (base_hbm, base_ref), (step_hbm, step_ref)]
        )
    ]
    for copy in copies:
        copy.start()
    copies[0].wait()
    blocks, block_len = col_ref.shape
    slots = blocks * block_len
    devices = req_ref.shape[0]
    cols = col_ref[...]
    owners = lax.shift_right_logical(cols, shift)
    local = (cols & ((1 << shift) - 1)) + 1
    owner_rows = iota((devices, block_len), 0)
    table = [one_hot(owner_rows == owners[k : k + 1, :]) for k in range(blocks)]
    table = jnp.concatenate(table, axis=1)
    earlier = one_hot(iota((slots, slots), 0) < iota((slots, slots), 1))
    counts = dot(table, earlier)
    ranked = jnp.sum(table.astype(F32) * counts, axis=0, keepdims=True).astype(jnp.int32)
    rank_rows = iota((LANES, block_len), 0)
    high, low = [], []
    for k in range(blocks):
        rank = ranked[:, k * block_len : (k + 1) * block_len]
        mine = rank_rows == rank
        value = local[k : k + 1, :]
        high.append(jnp.where(mine, lax.shift_right_logical(value, 5), 0).astype(F32))
        low.append(jnp.where(mine, value & 31, 0).astype(F32))
        pos_ref[k : k + 1, :] = owners[k : k + 1, :] * ROWS + rank
    high = jnp.concatenate(high, axis=1).astype(BF16)
    low = jnp.concatenate(low, axis=1).astype(BF16)
    nt = ((1,), (1,))
    req_ref[...] = (dot(table, high, nt) * 32.0 + dot(table, low, nt)).astype(jnp.int32) - 1
    copies[1].wait()
    copies[2].wait()
    jacobian = 1.0 + 0.5 * jnp.tanh(base_ref[...].astype(F32))
    form_ref[...] = (step_ref[...].astype(F32) * jacobian).astype(BF16)


def beta_rows(beta):
    high, low = split(beta)
    return jnp.concatenate([high.astype(F32), low.astype(F32)], axis=0).astype(BF16)


def second_kernel(
    after_ref,
    pos_ref,
    pred_ref,
    count_ref,
    beta_ref,
    weight_ref,
    coef_hbm,
    dep_hbm,
    slot_ref,
    norm_ref,
    base_ref,
    sums_ref,
    side_ref,
    stack_ref,
    coef,
    dep,
    scaled,
    coef_sem,
    dep_sem,
):
    blocks, npred, block_len = pred_ref.shape
    profile, _ = coef.shape
    slots = dep.shape[0]
    pieces = coef_sem.shape[0]
    size = profile // pieces

    def coef_copy(t):
        cut = pl.ds(t * size, size)
        return pltpu.make_async_copy(coef_hbm.at[cut], coef.at[cut], coef_sem.at[t])

    def dep_copy(t):
        part = pl.ds(t * (slots // dep_sem.shape[0]), slots // dep_sem.shape[0])
        return pltpu.make_async_copy(dep_hbm.at[part], dep.at[part], dep_sem.at[t])

    for t in range(pieces):
        coef_copy(t).start()
    for t in range(dep_sem.shape[0]):
        dep_copy(t).start()

    lane = iota((1, block_len), 1)
    stack = []
    for k in range(blocks):
        slot_ref[k : k + 1, :] = jnp.where(lane < count_ref[k], pos_ref[k : k + 1, :], -1)
        predictors = jnp.where(lane < count_ref[k], pred_ref[k], 0.0)
        high, low = split(predictors)
        high, low = high.astype(F32), low.astype(F32)
        stack.append(jnp.concatenate([high, low], axis=0))
        zeros = jnp.zeros((LANES - 4 * npred, block_len), F32)
        tall = jnp.concatenate([high, high, low, low, zeros], axis=0)
        side_ref[k * block_len : (k + 1) * block_len, :] = tall.T.astype(BF16)
    stack = jnp.concatenate(stack, axis=1).astype(BF16)
    stack_ref[...] = stack
    for t in range(pieces):
        coef_copy(t).wait()
        cut = slice(t * size, (t + 1) * size)
        scaled[cut, :] = (weight_ref[...] * coef[cut, :].astype(F32)).astype(BF16)
    nt = ((1,), (1,))
    rows = jnp.concatenate([coef[...], beta_rows(beta_ref[...])], axis=0)
    both = jnp.concatenate(split(dot(rows, scaled[...], nt)), axis=1)
    norm_ref[0 : profile + 2 * npred, :] = both
    norm_ref[profile + 2 * npred :, :] = both[profile:, :]
    for t in range(dep_sem.shape[0]):
        dep_copy(t).wait()
    base_ref[...] = dot(dep[...], scaled[...], nt)
    sums = dot(stack, dep[...])
    sums_ref[...] = sums[0:npred] + sums[npred:]


def owner_kernel(ids_ref, form_ref, out_hbm, pick, wide, out, sem):
    devices = ids_ref.shape[0]
    columns, profile = form_ref.shape
    cuts = profile // LANES
    group = RANKS * cuts
    lane = iota((devices, columns), 1)
    for r in range(RANKS):
        pick[r * devices : (r + 1) * devices, :] = one_hot(ids_ref[:, r : r + 1] == lane)
    result = dot(pick[...], form_ref[...])
    for r in range(RANKS):
        for c in range(cuts):
            wide[pl.ds(c * RANKS + r, devices, stride=group), :] = result[
                r * devices : (r + 1) * devices, c * LANES : (c + 1) * LANES
            ]
    out[...] = wide[...].astype(BF16)
    copy = pltpu.make_async_copy(out, out_hbm, sem)
    copy.start()
    copy.wait()


def main_kernel(
    arrived_ref,
    pos_ref,
    side_ref,
    stack_ref,
    norm_ref,
    base_ref,
    weight_ref,
    sums_ref,
    beta_ref,
    coef_hbm,
    out_hbm,
    left_ref,
    sums,
    turned,
    placed,
    coef,
    out,
    table,
    chosen,
    coef_sem,
    out_sem,
):
    blocks, block_len = pos_ref.shape
    rows, profile = out.shape
    npred, channels = sums.shape
    devices = rows // ROWS
    cuts = profile // LANES
    share = channels // devices
    depth = norm_ref.shape[0]
    coef_copy = pltpu.make_async_copy(coef_hbm, coef, coef_sem)
    coef_copy.start()

    count = devices * RANKS
    group = RANKS * cuts
    batch = 8

    def reorder(half, carry):
        for g in range(devices // batch // 2):
            at = half * (devices // batch // 2) + g
            start = pl.multiple_of(at * batch * group, 16)
            rows_in = arrived_ref[pl.ds(start, batch * group), :]
            here = pl.ds(pl.multiple_of(at * batch * RANKS, 16), batch * RANKS)
            for c in range(cuts):
                first = [d * group + c * RANKS for d in range(batch)]
                part = jnp.concatenate([rows_in[f : f + RANKS, :] for f in first], axis=0)
                table[here, c * LANES : (c + 1) * LANES] = part
        return carry

    lax.fori_loop(0, 2, reorder, 0)
    for k in range(blocks):
        here = pl.ds(k * block_len, block_len)
        row = pos_ref[k : k + 1, :]
        owner = lax.shift_right_arithmetic(row, ROWS.bit_length() - 1)
        row = jnp.where(row < 0, -1, row - owner * (ROWS - RANKS))
        column = jnp.broadcast_to(row.astype(F32), (block_len, block_len)).T.astype(jnp.int32)
        lane = iota((block_len, count), 1)
        chosen[here, :] = one_hot(jnp.concatenate([column] * (count // block_len), axis=1) == lane)
    left_ref[:, 0:profile] = dot(chosen[...], table[...]).astype(BF16)
    left_ref[:, profile:] = side_ref[...]
    left = left_ref[:, 0:depth]

    pulled = dot(left, norm_ref[...])
    pulled = (pulled[:, 0:profile] + pulled[:, profile:] - base_ref[...]).astype(BF16)
    step = rows // out_sem.shape[0]

    def copy(t):
        cut = pl.ds(t * step, step)
        return pltpu.make_async_copy(out.at[cut], out_hbm.at[cut], out_sem.at[t])

    for k in range(0, rows, step):
        index = iota((step, block_len), 0) + k
        place = [one_hot(index == pos_ref[b : b + 1, :]) for b in range(blocks)]
        placed[k : k + step, :] = dot(jnp.concatenate(place, axis=1), pulled)

    mixed = dot(stack_ref[...], left)
    high, low = split(mixed[0:npred] + mixed[npred:])
    mixed = jnp.concatenate([high.astype(F32), low.astype(F32)], axis=0).astype(BF16)
    tail = beta_rows(beta_ref[...])
    coef_copy.wait()
    mixed = dot(mixed, jnp.concatenate([coef[...], tail, tail], axis=0))
    sums[...] = weight_ref[...] * (mixed[0:npred] + mixed[npred:] - sums_ref[...])
    for d in range(devices):
        turned[d, :, 0:share] = sums[:, d * share : (d + 1) * share]
    bias = jnp.concatenate(
        [
            jnp.concatenate(
                [turned[:, p, 0:share], jnp.zeros((devices, PRED_STRIDE - share), F32)], axis=1
            )
            for p in range(npred)
        ],
        axis=1,
    )
    bias = jnp.concatenate(split(bias), axis=0)
    for k in range(0, rows, step):
        device = iota((step, devices), 1) * ROWS
        index = iota((step, devices), 0) + k
        place = [one_hot(index == device + (ROWS - 2)), one_hot(index == device + (ROWS - 1))]
        extra = dot(jnp.concatenate(place, axis=1), bias)
        out[k : k + step, :] = (placed[k : k + step, :] + extra).astype(BF16)
        copy(k // step).start()
    for k in range(rows // step):
        copy(k).wait()


def radiance_kernel(left_ref, beta_ref, coef_hbm, out_hbm, out, coef, sem, coef_sem):
    profile, channels = coef.shape
    npred = beta_ref.shape[0]
    depth = profile + 4 * npred
    steps = channels // TILE

    def copy(t):
        cut = pl.ds(t * TILE, TILE)
        return pltpu.make_async_copy(out.at[:, cut], out_hbm.at[:, cut], sem.at[t])

    coef_copy = pltpu.make_async_copy(coef_hbm, coef, coef_sem)
    coef_copy.start()
    tail = beta_rows(beta_ref[...])
    coef_copy.wait()
    for t in range(steps):
        cut = slice(t * TILE, (t + 1) * TILE)
        right = jnp.concatenate([coef[:, cut], tail[:, cut], tail[:, cut]], axis=0)
        out[:, cut] = dot(left_ref[:, 0:depth], right).astype(BF16)
        copy(t).start()
    for t in range(steps):
        copy(t).wait()


def final_kernel(ids_ref, base_ref, back_ref, grad_ref, bias_ref, *, scaling):
    devices = ids_ref.shape[0]
    columns = base_ref.shape[0]
    rows = back_ref.shape[0]
    npred, share = bias_ref.shape
    by_row = ids_ref[...].astype(F32).T[0:ROWS, :].astype(jnp.int32) + 1
    halves = jnp.concatenate(
        [lax.shift_right_logical(by_row, 5).astype(F32), (by_row & 31).astype(F32)], axis=0
    ).astype(BF16)
    spread = one_hot(lax.shift_right_logical(iota((devices, rows), 1), 3) == iota((devices, rows), 0))
    both = dot(halves, spread)
    both = both[0:ROWS] * 32.0 + both[ROWS:]
    mine = (iota((ROWS, rows), 1) & (ROWS - 1)) == iota((ROWS, rows), 0)
    wanted = jnp.sum(jnp.where(mine, both, 0.0), axis=0, keepdims=True).astype(jnp.int32) - 1
    step = 256
    for k in range(0, columns, step):
        place = one_hot(iota((step, rows), 0) + k == wanted)
        jacobian = 1.0 + 0.5 * jnp.tanh(base_ref[k : k + step, :].astype(F32))
        grad_ref[k : k + step, :] = (dot(place, back_ref[...]) * jacobian).astype(BF16)
    last = one_hot((iota((ROWS, rows), 1) & (ROWS - 1)) >= ROWS - 2)
    total = dot(last, back_ref[...])[0:1, :] * scaling
    for p in range(npred):
        bias_ref[p : p + 1, :] = total[:, p * PRED_STRIDE : p * PRED_STRIDE + share]


def exchange(x):
    return lax.all_to_all(x, AXES, split_axis=0, concat_axis=0, tiled=True)


def shards(
    background,
    increment,
    coefficients,
    departures,
    bias_pred,
    beta_incr,
    obs_weight,
    obs_count,
    col_index,
):
    devices = lax.axis_size(AXES)
    columns, profile = background.shape
    blocks, block_len = col_index.shape
    channels = coefficients.shape[1]
    npred = bias_pred.shape[2]
    slots = blocks * block_len
    rows = devices * ROWS
    shift = columns.bit_length() - 1
    assert columns == 1 << shift and channels % (TILE * 1) == 0
    scaling = float((slots * devices) ** -0.5)
    depth = profile + 4 * npred
    group = RANKS * profile // LANES

    def shape(*dims, dtype=BF16):
        return jax.ShapeDtypeStruct(dims, dtype)

    def call(kernel, outs, inputs, flops, in_specs=None, out_specs=None, scratch=(), vmem=None):
        return pl.pallas_call(
            kernel,
            out_shape=outs,
            in_specs=in_specs or [VMEM] * len(inputs),
            out_specs=out_specs or ([VMEM] * len(outs) if isinstance(outs, tuple) else VMEM),
            scratch_shapes=scratch,
            compiler_params=pltpu.CompilerParams(vmem_limit_bytes=vmem and vmem * 2**20),
            cost_estimate=pl.CostEstimate(
                flops=int(flops), bytes_accessed=4 * 2**20, transcendentals=0
            ),
        )(*inputs)

    def in_hbm(x):
        return pltpu.with_memory_space_constraint(x, pltpu.HBM)

    flat_dep = in_hbm(departures.reshape(slots, channels))
    coef_hbm = in_hbm(coefficients)
    requests, position, formed = call(
        lambda *refs: index_kernel(*refs, shift=shift),
        (
            shape(devices, LANES, dtype=jnp.int32),
            shape(blocks, block_len, dtype=jnp.int32),
            shape(columns, profile),
        ),
        (in_hbm(col_index), in_hbm(background), in_hbm(increment)),
        1e8,
        in_specs=[ANY] * 3,
        scratch=[
            pltpu.VMEM((blocks, block_len), jnp.int32),
            pltpu.VMEM((columns, profile), BF16),
            pltpu.VMEM((columns, profile), BF16),
            pltpu.SemaphoreType.DMA((3,)),
        ],
        vmem=16,
    )
    ids = exchange(requests.reshape(devices, 1, LANES)).reshape(devices, LANES)
    ids, obs_weight = lax.optimization_barrier((ids, obs_weight))
    weight = obs_weight.reshape(1, channels)
    rows_out = call(
        owner_kernel,
        shape(devices * group, LANES),
        (ids, formed),
        1e9,
        out_specs=ANY,
        scratch=[
            pltpu.VMEM((devices * RANKS, columns), BF16),
            pltpu.VMEM((devices * group, LANES), F32),
            pltpu.VMEM((devices * group, LANES), BF16),
            pltpu.SemaphoreType.DMA,
        ],
        vmem=16,
    )
    arrived = exchange(rows_out.reshape(devices, group // 2, 2, LANES))
    arrived = arrived.reshape(devices * group, LANES)
    slot_pos, norm, base, base_sums, side, stack = call(
        second_kernel,
        (
            shape(blocks, block_len, dtype=jnp.int32),
            shape(depth, 2 * profile),
            shape(slots, profile, dtype=F32),
            shape(npred, channels, dtype=F32),
            shape(slots, LANES),
            shape(2 * npred, slots),
        ),
        (
            ids,
            position,
            jnp.transpose(bias_pred, (0, 2, 1)),
            obs_count,
            beta_incr,
            weight,
            coef_hbm,
            flat_dep,
        ),
        8e9,
        in_specs=[ANY, VMEM, VMEM, SMEM, VMEM, VMEM, ANY, ANY],
        scratch=[
            pltpu.VMEM((profile, channels), BF16),
            pltpu.VMEM((slots, channels), BF16),
            pltpu.VMEM((profile, channels), BF16),
            pltpu.SemaphoreType.DMA((4,)),
            pltpu.SemaphoreType.DMA((4,)),
        ],
        vmem=32,
    )
    outgoing, left = call(
        main_kernel,
        (shape(rows, profile), shape(slots, profile + LANES)),
        (arrived, slot_pos, side, stack, norm, base, weight, base_sums, beta_incr, coef_hbm),
        2e9,
        in_specs=[VMEM] * 9 + [ANY],
        out_specs=(ANY, VMEM),
        scratch=[
            pltpu.VMEM((npred, channels), F32),
            pltpu.VMEM((devices, npred, LANES), F32),
            pltpu.VMEM((rows, profile), F32),
            pltpu.VMEM((profile, channels), BF16),
            pltpu.VMEM((rows, profile), BF16),
            pltpu.VMEM((devices * RANKS, profile), BF16),
            pltpu.VMEM((slots, devices * RANKS), BF16),
            pltpu.SemaphoreType.DMA,
            pltpu.SemaphoreType.DMA((4,)),
        ],
        vmem=24,
    )
    returned = exchange(outgoing.reshape(devices, ROWS, profile)).reshape(rows, profile)
    radiance = call(
        radiance_kernel,
        shape(slots, channels),
        (left, beta_incr, coef_hbm),
        3e9,
        in_specs=[VMEM, VMEM, ANY],
        out_specs=ANY,
        scratch=[
            pltpu.VMEM((slots, channels), BF16),
            pltpu.VMEM((profile, channels), BF16),
            pltpu.SemaphoreType.DMA((channels // TILE,)),
            pltpu.SemaphoreType.DMA,
        ],
        vmem=32,
    )
    column_grad, bias_grad = call(
        lambda *refs: final_kernel(*refs, scaling=scaling),
        (shape(columns, profile), shape(npred, channels // devices, dtype=F32)),
        (ids, background, returned),
        1e9,
        vmem=16,
    )
    return (
        radiance.reshape(blocks, block_len, channels),
        column_grad,
        jnp.transpose(bias_grad, (1, 0)),
    )


def solution(mesh):
    finer = Mesh(mesh.devices.reshape(4, 2, 4, 4), AXES)
    in_specs = (
        P(AXES, None),
        P(AXES, None),
        P(),
        P(AXES, None, None),
        P(AXES, None, None),
        P(),
        P(),
        P(AXES),
        P(AXES, None),
    )
    out_specs = (P(AXES, None, None), P(AXES, None), P(AXES, None))
    return jax.shard_map(
        shards, mesh=finer, in_specs=in_specs, out_specs=out_specs, check_vma=False
    )
```

```python
import jax
import jax.numpy as jnp
from jax import lax
from jax.experimental import pallas as pl
from jax.experimental.pallas import tpu as pltpu
from jax.sharding import Mesh
from jax.sharding import PartitionSpec as P

AXES = ("lat_0", "lat_1", "lon_0", "lon_1")
RANKS = 6
ROWS = 8
LANES = 128
BIAS_ROWS = 4
TILE = 256
F32 = jnp.float32
BF16 = jnp.bfloat16
VMEM = pl.BlockSpec(memory_space=pltpu.VMEM)
SMEM = pl.BlockSpec(memory_space=pltpu.SMEM)
ANY = pl.BlockSpec(memory_space=pl.ANY)


def iota(shape, dim):
    return lax.broadcasted_iota(jnp.int32, shape, dim)


def one_hot(mask):
    return jnp.where(mask, 1.0, 0.0).astype(BF16)


def dot(a, b, dims=((1,), (0,))):
    return lax.dot_general(a, b, (dims, ((), ())), preferred_element_type=F32)


def split(x):
    high = x.astype(BF16)
    return high, (x - high.astype(F32)).astype(BF16)


def index_kernel(
    col_hbm, base_hbm, step_hbm, req_ref, pos_ref, form_ref, col_ref, base_ref, step_ref, sem, *, shift
):
    copies = [
        pltpu.make_async_copy(source, target, sem.at[k])
        for k, (source, target) in enumerate(
            [(col_hbm, col_ref), (base_hbm, base_ref), (step_hbm, step_ref)]
        )
    ]
    for copy in copies:
        copy.start()
    copies[0].wait()
    blocks, block_len = col_ref.shape
    slots = blocks * block_len
    devices = req_ref.shape[0]
    cols = col_ref[...]
    owners = lax.shift_right_logical(cols, shift)
    local = (cols & ((1 << shift) - 1)) + 1
    owner_rows = iota((devices, block_len), 0)
    table = [one_hot(owner_rows == owners[k : k + 1, :]) for k in range(blocks)]
    table = jnp.concatenate(table, axis=1)
    earlier = one_hot(iota((slots, slots), 0) < iota((slots, slots), 1))
    counts = dot(table, earlier)
    ranked = jnp.sum(table.astype(F32) * counts, axis=0, keepdims=True).astype(jnp.int32)
    rank_rows = iota((LANES, block_len), 0)
    high, low = [], []
    for k in range(blocks):
        rank = ranked[:, k * block_len : (k + 1) * block_len]
        mine = rank_rows == rank
        value = local[k : k + 1, :]
        high.append(jnp.where(mine, lax.shift_right_logical(value, 5), 0).astype(F32))
        low.append(jnp.where(mine, value & 31, 0).astype(F32))
        pos_ref[k : k + 1, :] = owners[k : k + 1, :] * ROWS + rank
    high = jnp.concatenate(high, axis=1).astype(BF16)
    low = jnp.concatenate(low, axis=1).astype(BF16)
    nt = ((1,), (1,))
    req_ref[...] = (dot(table, high, nt) * 32.0 + dot(table, low, nt)).astype(jnp.int32) - 1
    copies[1].wait()
    copies[2].wait()
    jacobian = 1.0 + 0.5 * jnp.tanh(base_ref[...].astype(F32))
    form_ref[...] = (step_ref[...].astype(F32) * jacobian).astype(BF16)


def beta_rows(beta):
    high, low = split(beta)
    return jnp.concatenate([high.astype(F32), low.astype(F32)], axis=0).astype(BF16)


def second_kernel(
    after_ref,
    pos_ref,
    pred_ref,
    count_ref,
    beta_ref,
    weight_ref,
    coef_hbm,
    dep_hbm,
    slot_ref,
    norm_ref,
    base_ref,
    sums_ref,
    side_ref,
    stack_ref,
    coef,
    dep,
    scaled,
    coef_sem,
    dep_sem,
):
    blocks, npred, block_len = pred_ref.shape
    profile, _ = coef.shape
    slots = dep.shape[0]
    pieces = coef_sem.shape[0]
    size = profile // pieces

    def coef_copy(t):
        cut = pl.ds(t * size, size)
        return pltpu.make_async_copy(coef_hbm.at[cut], coef.at[cut], coef_sem.at[t])

    def dep_copy(t):
        part = pl.ds(t * (slots // dep_sem.shape[0]), slots // dep_sem.shape[0])
        return pltpu.make_async_copy(dep_hbm.at[part], dep.at[part], dep_sem.at[t])

    for t in range(pieces):
        coef_copy(t).start()
    for t in range(dep_sem.shape[0]):
        dep_copy(t).start()

    lane = iota((1, block_len), 1)
    stack = []
    for k in range(blocks):
        slot_ref[k : k + 1, :] = jnp.where(lane < count_ref[k], pos_ref[k : k + 1, :], -1)
        predictors = jnp.where(lane < count_ref[k], pred_ref[k], 0.0)
        high, low = split(predictors)
        high, low = high.astype(F32), low.astype(F32)
        stack.append(jnp.concatenate([high, low], axis=0))
        zeros = jnp.zeros((LANES - 4 * npred, block_len), F32)
        tall = jnp.concatenate([high, high, low, low, zeros], axis=0)
        side_ref[k * block_len : (k + 1) * block_len, :] = tall.T.astype(BF16)
    stack = jnp.concatenate(stack, axis=1).astype(BF16)
    stack_ref[...] = stack
    for t in range(pieces):
        coef_copy(t).wait()
        cut = slice(t * size, (t + 1) * size)
        scaled[cut, :] = (weight_ref[...] * coef[cut, :].astype(F32)).astype(BF16)
    nt = ((1,), (1,))
    rows = jnp.concatenate([coef[...], beta_rows(beta_ref[...])], axis=0)
    both = jnp.concatenate(split(dot(rows, scaled[...], nt)), axis=1)
    norm_ref[0 : profile + 2 * npred, :] = both
    norm_ref[profile + 2 * npred :, :] = both[profile:, :]
    for t in range(dep_sem.shape[0]):
        dep_copy(t).wait()
    base_ref[...] = dot(dep[...], scaled[...], nt)
    sums = dot(stack, dep[...])
    sums_ref[...] = sums[0:npred] + sums[npred:]


def owner_kernel(ids_ref, form_ref, out_hbm, pick, wide, out, sem):
    devices = ids_ref.shape[0]
    columns, profile = form_ref.shape
    cuts = profile // LANES
    group = RANKS * cuts
    lane = iota((devices, columns), 1)
    for r in range(RANKS):
        pick[r * devices : (r + 1) * devices, :] = one_hot(ids_ref[:, r : r + 1] == lane)
    result = dot(pick[...], form_ref[...])
    for r in range(RANKS):
        for c in range(cuts):
            wide[pl.ds(c * RANKS + r, devices, stride=group), :] = result[
                r * devices : (r + 1) * devices, c * LANES : (c + 1) * LANES
            ]
    out[...] = wide[...].astype(BF16)
    copy = pltpu.make_async_copy(out, out_hbm, sem)
    copy.start()
    copy.wait()


def reorder(ref, table, group, turns):
    count, profile = table.shape
    cuts = profile // LANES
    devices = count // RANKS
    batch = 8

    def turn(index, carry):
        for g in range(devices // batch // turns):
            at = index * (devices // batch // turns) + g
            start = pl.multiple_of(at * batch * group, 16)
            rows_in = ref[pl.ds(start, batch * group), :]
            here = pl.ds(pl.multiple_of(at * batch * RANKS, 16), batch * RANKS)
            for c in range(cuts):
                first = [d * group + c * RANKS for d in range(batch)]
                part = jnp.concatenate([rows_in[f : f + RANKS, :] for f in first], axis=0)
                table[here, c * LANES : (c + 1) * LANES] = part
        return carry

    lax.fori_loop(0, turns, turn, 0)


def main_kernel(
    arrived_ref,
    pos_ref,
    side_ref,
    stack_ref,
    norm_ref,
    base_ref,
    weight_ref,
    sums_ref,
    beta_ref,
    coef_hbm,
    out_hbm,
    left_hbm,
    left_ref,
    sums,
    turned,
    wide,
    coef,
    out,
    table,
    chosen,
    coef_sem,
    out_sem,
    left_sem,
):
    blocks, block_len = pos_ref.shape
    profile = coef.shape[0]
    npred, channels = sums.shape
    devices = turned.shape[0]
    cuts = profile // LANES
    share = channels // devices
    depth = norm_ref.shape[0]
    coef_copy = pltpu.make_async_copy(coef_hbm, coef, coef_sem)
    coef_copy.start()

    count = devices * RANKS
    group = RANKS * cuts
    reorder(arrived_ref, table, group, 2)
    below = []
    for k in range(blocks):
        here = pl.ds(k * block_len, block_len)
        row = pos_ref[k : k + 1, :]
        owner = lax.shift_right_arithmetic(row, ROWS.bit_length() - 1)
        below.append(jnp.where(row < 0, -1, (row & (ROWS - 1)) * devices + owner))
        row = jnp.where(row < 0, -1, row - owner * (ROWS - RANKS))
        column = jnp.broadcast_to(row.astype(F32), (block_len, block_len)).T.astype(jnp.int32)
        lane = iota((block_len, count), 1)
        chosen[here, :] = one_hot(jnp.concatenate([column] * (count // block_len), axis=1) == lane)
    left_ref[:, 0:profile] = dot(chosen[...], table[...]).astype(BF16)
    left_ref[:, profile:] = side_ref[...]
    left_copy = pltpu.make_async_copy(left_ref, left_hbm, left_sem)
    left_copy.start()
    left = left_ref[:, 0:depth]

    pulled = dot(left, norm_ref[...])
    pulled = (pulled[:, 0:profile] + pulled[:, profile:] - base_ref[...]).astype(BF16)
    chunk = group + BIAS_ROWS
    step = 256
    for k in range(0, count, step):
        index = iota((step, block_len), 0) + k
        place = jnp.concatenate([one_hot(index == row) for row in below], axis=1)
        placed = dot(place, pulled)
        for r in range(k // devices, (k + step) // devices):
            for c in range(cuts):
                wide[pl.ds(c * RANKS + r, devices, stride=chunk), :] = placed[
                    r * devices - k : (r + 1) * devices - k, c * LANES : (c + 1) * LANES
                ]

    mixed = dot(stack_ref[...], left)
    high, low = split(mixed[0:npred] + mixed[npred:])
    mixed = jnp.concatenate([high.astype(F32), low.astype(F32)], axis=0).astype(BF16)
    tail = beta_rows(beta_ref[...])
    coef_copy.wait()
    mixed = dot(mixed, jnp.concatenate([coef[...], tail, tail], axis=0))
    sums[...] = weight_ref[...] * (mixed[0:npred] + mixed[npred:] - sums_ref[...])
    for d in range(devices):
        turned[d, :, 0:share] = sums[:, d * share : (d + 1) * share]
    bias = jnp.concatenate([turned[:, p, 0:share] for p in range(npred)], axis=1)
    high = bias.astype(BF16).astype(F32)
    spare = BIAS_ROWS * LANES - npred * share
    both = jnp.concatenate([high, (bias - high)[:, 0:spare]], axis=1)
    for q in range(BIAS_ROWS):
        part = both[:, q * LANES : (q + 1) * LANES]
        wide[pl.ds(group + q, devices, stride=chunk), :] = part
    out[...] = wide[...].astype(BF16)
    copy = pltpu.make_async_copy(out, out_hbm, out_sem)
    copy.start()
    left_copy.wait()
    copy.wait()


def radiance_kernel(left_ref, beta_ref, coef_hbm, out_hbm, out, coef, sem, coef_sem):
    profile, channels = coef.shape
    npred = beta_ref.shape[0]
    depth = profile + 4 * npred
    steps = channels // TILE

    def copy(t):
        cut = pl.ds(t * TILE, TILE)
        return pltpu.make_async_copy(out.at[:, cut], out_hbm.at[:, cut], sem.at[t])

    coef_copy = pltpu.make_async_copy(coef_hbm, coef, coef_sem)
    coef_copy.start()
    tail = beta_rows(beta_ref[...])
    coef_copy.wait()
    for t in range(steps):
        cut = slice(t * TILE, (t + 1) * TILE)
        right = jnp.concatenate([coef[:, cut], tail[:, cut], tail[:, cut]], axis=0)
        out[:, cut] = dot(left_ref[:, 0:depth], right).astype(BF16)
        copy(t).start()
    for t in range(steps):
        copy(t).wait()


def groups_of(shape, dim, size):
    index = iota(shape, dim)
    group = jnp.floor((index.astype(F32) + 0.5) * (1.0 / size)).astype(jnp.int32)
    return group, index - group * size


def target_kernel(ids_ref, after_ref, place_ref):
    devices = ids_ref.shape[0]
    columns, count = place_ref.shape
    by_row = ids_ref[...].astype(F32).T[0:ROWS, :].astype(jnp.int32) + 1
    halves = jnp.concatenate(
        [lax.shift_right_logical(by_row, 5).astype(F32), (by_row & 31).astype(F32)], axis=0
    ).astype(BF16)
    owner, _ = groups_of((devices, count), 1, RANKS)
    both = dot(halves, one_hot(owner == iota((devices, count), 0)))
    both = both[0:ROWS] * 32.0 + both[ROWS:]
    _, rank = groups_of((ROWS, count), 1, RANKS)
    mine = rank == iota((ROWS, count), 0)
    wanted = jnp.sum(jnp.where(mine, both, 0.0), axis=0, keepdims=True).astype(jnp.int32) - 1
    step = 256
    for k in range(0, columns, step):
        place_ref[k : k + step, :] = one_hot(iota((step, count), 0) + k == wanted)


def final_kernel(place_ref, base_ref, back_ref, grad_ref, bias_ref, table, *, scaling):
    columns, count = place_ref.shape
    devices = count // RANKS
    rows = back_ref.shape[0]
    chunk = rows // devices
    npred, share = bias_ref.shape
    _, inside = groups_of((ROWS, rows), 1, chunk)
    last = one_hot(inside == iota((ROWS, rows), 0) + (chunk - BIAS_ROWS))
    total = dot(last, back_ref[...])
    total = jnp.concatenate([total[q : q + 1, :] for q in range(BIAS_ROWS)], axis=1)
    high, low = total[:, 0 : npred * share], total[:, npred * share :]
    spare = npred * share - low.shape[1]
    total = (high + jnp.concatenate([low, jnp.zeros((1, spare), F32)], axis=1)) * scaling
    for p in range(npred):
        bias_ref[p : p + 1, :] = total[:, p * share : (p + 1) * share]
    reorder(back_ref, table, chunk, 1)
    step = 256
    for k in range(0, columns, step):
        jacobian = 1.0 + 0.5 * jnp.tanh(base_ref[k : k + step, :].astype(F32))
        grad = dot(place_ref[k : k + step, :], table[...]) * jacobian
        grad_ref[k : k + step, :] = grad.astype(BF16)


def exchange(x):
    return lax.all_to_all(x, AXES, split_axis=0, concat_axis=0, tiled=True)


def shards(
    background,
    increment,
    coefficients,
    departures,
    bias_pred,
    beta_incr,
    obs_weight,
    obs_count,
    col_index,
):
    devices = lax.axis_size(AXES)
    columns, profile = background.shape
    blocks, block_len = col_index.shape
    channels = coefficients.shape[1]
    npred = bias_pred.shape[2]
    slots = blocks * block_len
    shift = columns.bit_length() - 1
    assert columns == 1 << shift and channels % (TILE * 1) == 0
    scaling = float((slots * devices) ** -0.5)
    depth = profile + 4 * npred
    group = RANKS * profile // LANES
    chunk = group + BIAS_ROWS

    def shape(*dims, dtype=BF16):
        return jax.ShapeDtypeStruct(dims, dtype)

    def call(kernel, outs, inputs, flops, in_specs=None, out_specs=None, scratch=(), vmem=None):
        return pl.pallas_call(
            kernel,
            out_shape=outs,
            in_specs=in_specs or [VMEM] * len(inputs),
            out_specs=out_specs or ([VMEM] * len(outs) if isinstance(outs, tuple) else VMEM),
            scratch_shapes=scratch,
            compiler_params=pltpu.CompilerParams(vmem_limit_bytes=vmem and vmem * 2**20),
            cost_estimate=pl.CostEstimate(
                flops=int(flops), bytes_accessed=4 * 2**20, transcendentals=0
            ),
        )(*inputs)

    def in_hbm(x):
        return pltpu.with_memory_space_constraint(x, pltpu.HBM)

    flat_dep = in_hbm(departures.reshape(slots, channels))
    coef_hbm = in_hbm(coefficients)
    requests, position, formed = call(
        lambda *refs: index_kernel(*refs, shift=shift),
        (
            shape(devices, LANES, dtype=jnp.int32),
            shape(blocks, block_len, dtype=jnp.int32),
            shape(columns, profile),
        ),
        (in_hbm(col_index), in_hbm(background), in_hbm(increment)),
        1e8,
        in_specs=[ANY] * 3,
        scratch=[
            pltpu.VMEM((blocks, block_len), jnp.int32),
            pltpu.VMEM((columns, profile), BF16),
            pltpu.VMEM((columns, profile), BF16),
            pltpu.SemaphoreType.DMA((3,)),
        ],
        vmem=16,
    )
    ids = exchange(requests.reshape(devices, 1, LANES)).reshape(devices, LANES)
    ids, obs_weight = lax.optimization_barrier((ids, obs_weight))
    weight = obs_weight.reshape(1, channels)
    rows_out = call(
        owner_kernel,
        shape(devices * group, LANES),
        (ids, formed),
        1e9,
        out_specs=ANY,
        scratch=[
            pltpu.VMEM((devices * RANKS, columns), BF16),
            pltpu.VMEM((devices * group, LANES), F32),
            pltpu.VMEM((devices * group, LANES), BF16),
            pltpu.SemaphoreType.DMA,
        ],
        vmem=16,
    )
    arrived = exchange(rows_out.reshape(devices, group // 2, 2, LANES))
    arrived = arrived.reshape(devices * group, LANES)
    slot_pos, norm, base, base_sums, side, stack = call(
        second_kernel,
        (
            shape(blocks, block_len, dtype=jnp.int32),
            shape(depth, 2 * profile),
            shape(slots, profile, dtype=F32),
            shape(npred, channels, dtype=F32),
            shape(slots, LANES),
            shape(2 * npred, slots),
        ),
        (
            ids,
            position,
            jnp.transpose(bias_pred, (0, 2, 1)),
            obs_count,
            beta_incr,
            weight,
            coef_hbm,
            flat_dep,
        ),
        8e9,
        in_specs=[ANY, VMEM, VMEM, SMEM, VMEM, VMEM, ANY, ANY],
        scratch=[
            pltpu.VMEM((profile, channels), BF16),
            pltpu.VMEM((slots, channels), BF16),
            pltpu.VMEM((profile, channels), BF16),
            pltpu.SemaphoreType.DMA((4,)),
            pltpu.SemaphoreType.DMA((4,)),
        ],
        vmem=32,
    )
    outgoing, left = call(
        main_kernel,
        (
            shape(devices * chunk, LANES),
            pltpu.HBM((slots, profile + LANES), BF16),
        ),
        (arrived, slot_pos, side, stack, norm, base, weight, base_sums, beta_incr, coef_hbm),
        2e9,
        in_specs=[VMEM] * 9 + [ANY],
        out_specs=(ANY, ANY),
        scratch=[
            pltpu.VMEM((slots, profile + LANES), BF16),
            pltpu.VMEM((npred, channels), F32),
            pltpu.VMEM((devices, npred, LANES), F32),
            pltpu.VMEM((devices * chunk, LANES), F32),
            pltpu.VMEM((profile, channels), BF16),
            pltpu.VMEM((devices * chunk, LANES), BF16),
            pltpu.VMEM((devices * RANKS, profile), BF16),
            pltpu.VMEM((slots, devices * RANKS), BF16),
            pltpu.SemaphoreType.DMA,
            pltpu.SemaphoreType.DMA,
            pltpu.SemaphoreType.DMA,
        ],
        vmem=24,
    )
    returned = exchange(outgoing.reshape(devices, chunk // 2, 2, LANES))
    returned = returned.reshape(devices * chunk, LANES)
    place = call(
        target_kernel,
        shape(columns, devices * RANKS),
        (ids, in_hbm(left)),
        1e9,
        in_specs=[VMEM, ANY],
        vmem=16,
    )
    radiance = call(
        radiance_kernel,
        shape(slots, channels),
        (left, beta_incr, coef_hbm),
        3e9,
        in_specs=[VMEM, VMEM, ANY],
        out_specs=ANY,
        scratch=[
            pltpu.VMEM((slots, channels), BF16),
            pltpu.VMEM((profile, channels), BF16),
            pltpu.SemaphoreType.DMA((channels // TILE,)),
            pltpu.SemaphoreType.DMA,
        ],
        vmem=32,
    )
    column_grad, bias_grad = call(
        lambda *refs: final_kernel(*refs, scaling=scaling),
        (shape(columns, profile), shape(npred, channels // devices, dtype=F32)),
        (place, background, returned),
        1e9,
        scratch=[pltpu.VMEM((devices * RANKS, profile), BF16)],
        vmem=16,
    )
    return (
        radiance.reshape(blocks, block_len, channels),
        column_grad,
        jnp.transpose(bias_grad, (1, 0)),
    )


def solution(mesh):
    finer = Mesh(mesh.devices.reshape(4, 2, 4, 4), AXES)
    in_specs = (
        P(AXES, None),
        P(AXES, None),
        P(),
        P(AXES, None, None),
        P(AXES, None, None),
        P(),
        P(),
        P(AXES),
        P(AXES, None),
    )
    out_specs = (P(AXES, None, None), P(AXES, None), P(AXES, None))
    return jax.shard_map(
        shards, mesh=finer, in_specs=in_specs, out_specs=out_specs, check_vma=False
    )
```

```python
import jax
import jax.numpy as jnp
from jax import lax
from jax.experimental import pallas as pl
from jax.experimental.pallas import tpu as pltpu
from jax.sharding import Mesh
from jax.sharding import PartitionSpec as P

AXES = ("lat_0", "lat_1", "lon_0", "lon_1")
RANKS = 6
ROWS = 8
LANES = 128
BIAS_ROWS = 4
TILE = 256
F32 = jnp.float32
BF16 = jnp.bfloat16
VMEM = pl.BlockSpec(memory_space=pltpu.VMEM)
SMEM = pl.BlockSpec(memory_space=pltpu.SMEM)
ANY = pl.BlockSpec(memory_space=pl.ANY)


def iota(shape, dim):
    return lax.broadcasted_iota(jnp.int32, shape, dim)


def one_hot(mask):
    return jnp.where(mask, 1.0, 0.0).astype(BF16)


def dot(a, b, dims=((1,), (0,))):
    return lax.dot_general(a, b, (dims, ((), ())), preferred_element_type=F32)


def split(x):
    high = x.astype(BF16)
    return high, (x - high.astype(F32)).astype(BF16)


def index_kernel(
    col_hbm, base_hbm, step_hbm, req_ref, pos_ref, form_ref, col_ref, base_ref, step_ref, sem, *, shift
):
    parts = (sem.shape[0] - 1) // 2
    size = base_ref.shape[0] // parts
    copies = [pltpu.make_async_copy(col_hbm, col_ref, sem.at[0])]
    for t in range(parts):
        cut = pl.ds(t * size, size)
        copies += [
            pltpu.make_async_copy(base_hbm.at[cut], base_ref.at[cut], sem.at[2 * t + 1]),
            pltpu.make_async_copy(step_hbm.at[cut], step_ref.at[cut], sem.at[2 * t + 2]),
        ]
    for copy in copies:
        copy.start()
    copies[0].wait()
    blocks, block_len = col_ref.shape
    slots = blocks * block_len
    devices = req_ref.shape[0]
    cols = col_ref[...]
    owners = lax.shift_right_logical(cols, shift)
    local = (cols & ((1 << shift) - 1)) + 1
    owner_rows = iota((devices, block_len), 0)
    table = [one_hot(owner_rows == owners[k : k + 1, :]) for k in range(blocks)]
    table = jnp.concatenate(table, axis=1)
    earlier = one_hot(iota((slots, slots), 0) < iota((slots, slots), 1))
    counts = dot(table, earlier)
    ranked = jnp.sum(table.astype(F32) * counts, axis=0, keepdims=True).astype(jnp.int32)
    rank_rows = iota((LANES, block_len), 0)
    high, low = [], []
    for k in range(blocks):
        rank = ranked[:, k * block_len : (k + 1) * block_len]
        mine = rank_rows == rank
        value = local[k : k + 1, :]
        high.append(jnp.where(mine, lax.shift_right_logical(value, 5), 0).astype(F32))
        low.append(jnp.where(mine, value & 31, 0).astype(F32))
        pos_ref[k : k + 1, :] = owners[k : k + 1, :] * ROWS + rank
    high = jnp.concatenate(high, axis=1).astype(BF16)
    low = jnp.concatenate(low, axis=1).astype(BF16)
    nt = ((1,), (1,))
    req_ref[...] = (dot(table, high, nt) * 32.0 + dot(table, low, nt)).astype(jnp.int32) - 1
    for t in range(parts):
        copies[2 * t + 1].wait()
        copies[2 * t + 2].wait()
        cut = slice(t * size, (t + 1) * size)
        jacobian = 1.0 + 0.5 * jnp.tanh(base_ref[cut, :].astype(F32))
        form_ref[cut, :] = (step_ref[cut, :].astype(F32) * jacobian).astype(BF16)


def beta_rows(beta):
    high, low = split(beta)
    return jnp.concatenate([high.astype(F32), low.astype(F32)], axis=0).astype(BF16)


def second_kernel(
    after_ref,
    pos_ref,
    pred_ref,
    count_ref,
    beta_ref,
    weight_ref,
    coef_hbm,
    dep_hbm,
    slot_ref,
    norm_ref,
    base_ref,
    sums_ref,
    side_ref,
    stack_ref,
    coef,
    dep,
    scaled,
    coef_sem,
    dep_sem,
):
    blocks, npred, block_len = pred_ref.shape
    profile, _ = coef.shape
    slots = dep.shape[0]
    pieces = coef_sem.shape[0]
    size = profile // pieces

    def coef_copy(t):
        cut = pl.ds(t * size, size)
        return pltpu.make_async_copy(coef_hbm.at[cut], coef.at[cut], coef_sem.at[t])

    def dep_copy(t):
        part = pl.ds(t * (slots // dep_sem.shape[0]), slots // dep_sem.shape[0])
        return pltpu.make_async_copy(dep_hbm.at[part], dep.at[part], dep_sem.at[t])

    for t in range(pieces):
        coef_copy(t).start()
    for t in range(dep_sem.shape[0]):
        dep_copy(t).start()

    lane = iota((1, block_len), 1)
    stack = []
    for k in range(blocks):
        slot_ref[k : k + 1, :] = jnp.where(lane < count_ref[k], pos_ref[k : k + 1, :], -1)
        predictors = jnp.where(lane < count_ref[k], pred_ref[k], 0.0)
        high, low = split(predictors)
        high, low = high.astype(F32), low.astype(F32)
        stack.append(jnp.concatenate([high, low], axis=0))
        zeros = jnp.zeros((LANES - 4 * npred, block_len), F32)
        tall = jnp.concatenate([high, high, low, low, zeros], axis=0)
        side_ref[k * block_len : (k + 1) * block_len, :] = tall.T.astype(BF16)
    stack = jnp.concatenate(stack, axis=1).astype(BF16)
    stack_ref[...] = stack
    for t in range(pieces):
        coef_copy(t).wait()
        cut = slice(t * size, (t + 1) * size)
        scaled[cut, :] = (weight_ref[...] * coef[cut, :].astype(F32)).astype(BF16)
    nt = ((1,), (1,))
    rows = jnp.concatenate([coef[...], beta_rows(beta_ref[...])], axis=0)
    both = jnp.concatenate(split(dot(rows, scaled[...], nt)), axis=1)
    norm_ref[0 : profile + 2 * npred, :] = both
    norm_ref[profile + 2 * npred :, :] = both[profile:, :]
    for t in range(dep_sem.shape[0]):
        dep_copy(t).wait()
    base_ref[...] = dot(dep[...], scaled[...], nt)
    sums = dot(stack, dep[...])
    sums_ref[...] = sums[0:npred] + sums[npred:]


def store_halves(wide, out, out_hbm, sem):
    half = out.shape[0] // 2
    copies = []
    for t in range(2):
        cut = pl.ds(t * half, half)
        out[cut, :] = wide[cut, :].astype(BF16)
        copies.append(pltpu.make_async_copy(out.at[cut], out_hbm.at[cut], sem.at[t]))
        copies[t].start()
    return copies


def owner_kernel(ids_ref, form_ref, out_hbm, pick, wide, out, sem):
    devices = ids_ref.shape[0]
    columns, profile = form_ref.shape
    cuts = profile // LANES
    group = RANKS * cuts
    lane = iota((devices, columns), 1)
    for r in range(RANKS):
        pick[r * devices : (r + 1) * devices, :] = one_hot(ids_ref[:, r : r + 1] == lane)
    result = dot(pick[...], form_ref[...])
    for r in range(RANKS):
        for c in range(cuts):
            wide[pl.ds(c * RANKS + r, devices, stride=group), :] = result[
                r * devices : (r + 1) * devices, c * LANES : (c + 1) * LANES
            ]
    copies = store_halves(wide, out, out_hbm, sem)
    for copy in copies:
        copy.wait()


def reorder(ref, table, group, turns):
    count, profile = table.shape
    cuts = profile // LANES
    devices = count // RANKS
    batch = 8

    def turn(index, carry):
        for g in range(devices // batch // turns):
            at = index * (devices // batch // turns) + g
            start = pl.multiple_of(at * batch * group, 16)
            rows_in = ref[pl.ds(start, batch * group), :]
            here = pl.ds(pl.multiple_of(at * batch * RANKS, 16), batch * RANKS)
            for c in range(cuts):
                first = [d * group + c * RANKS for d in range(batch)]
                part = jnp.concatenate([rows_in[f : f + RANKS, :] for f in first], axis=0)
                table[here, c * LANES : (c + 1) * LANES] = part
        return carry

    lax.fori_loop(0, turns, turn, 0)


def main_kernel(
    arrived_ref,
    pos_ref,
    side_ref,
    stack_ref,
    norm_ref,
    base_ref,
    weight_ref,
    sums_ref,
    beta_ref,
    coef_hbm,
    out_hbm,
    left_hbm,
    left_ref,
    sums,
    turned,
    wide,
    coef,
    out,
    table,
    chosen,
    coef_sem,
    out_sem,
    left_sem,
):
    blocks, block_len = pos_ref.shape
    profile = coef.shape[0]
    npred, channels = sums.shape
    devices = turned.shape[0]
    cuts = profile // LANES
    share = channels // devices
    depth = norm_ref.shape[0]
    coef_copy = pltpu.make_async_copy(coef_hbm, coef, coef_sem)
    coef_copy.start()

    count = devices * RANKS
    group = RANKS * cuts
    reorder(arrived_ref, table, group, 2)
    below = []
    for k in range(blocks):
        here = pl.ds(k * block_len, block_len)
        row = pos_ref[k : k + 1, :]
        owner = lax.shift_right_arithmetic(row, ROWS.bit_length() - 1)
        below.append(jnp.where(row < 0, -1, (row & (ROWS - 1)) * devices + owner))
        row = jnp.where(row < 0, -1, row - owner * (ROWS - RANKS))
        column = jnp.broadcast_to(row.astype(F32), (block_len, block_len)).T.astype(jnp.int32)
        lane = iota((block_len, count), 1)
        chosen[here, :] = one_hot(jnp.concatenate([column] * (count // block_len), axis=1) == lane)
    left_ref[:, 0:profile] = dot(chosen[...], table[...]).astype(BF16)
    left_ref[:, profile:] = side_ref[...]
    left_copy = pltpu.make_async_copy(left_ref, left_hbm, left_sem)
    left_copy.start()
    left = left_ref[:, 0:depth]

    pulled = dot(left, norm_ref[...])
    pulled = (pulled[:, 0:profile] + pulled[:, profile:] - base_ref[...]).astype(BF16)
    chunk = group + BIAS_ROWS
    step = 256
    coef_copy.wait()
    for k in range(0, count, step):
        index = iota((step, block_len), 0) + k
        place = jnp.concatenate([one_hot(index == row) for row in below], axis=1)
        placed = dot(place, pulled)
        for r in range(k // devices, (k + step) // devices):
            for c in range(cuts):
                wide[pl.ds(c * RANKS + r, devices, stride=chunk), :] = placed[
                    r * devices - k : (r + 1) * devices - k, c * LANES : (c + 1) * LANES
                ]

    mixed = dot(stack_ref[...], left)
    high, low = split(mixed[0:npred] + mixed[npred:])
    mixed = jnp.concatenate([high.astype(F32), low.astype(F32)], axis=0).astype(BF16)
    tail = beta_rows(beta_ref[...])
    mixed = dot(mixed, jnp.concatenate([coef[...], tail, tail], axis=0))
    sums[...] = weight_ref[...] * (mixed[0:npred] + mixed[npred:] - sums_ref[...])
    for d in range(devices):
        turned[d, :, 0:share] = sums[:, d * share : (d + 1) * share]
    bias = jnp.concatenate([turned[:, p, 0:share] for p in range(npred)], axis=1)
    high = bias.astype(BF16).astype(F32)
    spare = BIAS_ROWS * LANES - npred * share
    both = jnp.concatenate([high, (bias - high)[:, 0:spare]], axis=1)
    for q in range(BIAS_ROWS):
        part = both[:, q * LANES : (q + 1) * LANES]
        wide[pl.ds(group + q, devices, stride=chunk), :] = part
    copies = store_halves(wide, out, out_hbm, out_sem)
    for copy in copies + [left_copy]:
        copy.wait()


def radiance_kernel(left_ref, beta_ref, coef_hbm, out_hbm, out, coef, sem, coef_sem):
    profile, channels = coef.shape
    npred = beta_ref.shape[0]
    depth = profile + 4 * npred
    steps = channels // TILE

    def copy(t):
        cut = pl.ds(t * TILE, TILE)
        return pltpu.make_async_copy(out.at[:, cut], out_hbm.at[:, cut], sem.at[t])

    coef_copy = pltpu.make_async_copy(coef_hbm, coef, coef_sem)
    coef_copy.start()
    tail = beta_rows(beta_ref[...])
    coef_copy.wait()
    for t in range(steps):
        cut = slice(t * TILE, (t + 1) * TILE)
        right = jnp.concatenate([coef[:, cut], tail[:, cut], tail[:, cut]], axis=0)
        out[:, cut] = dot(left_ref[:, 0:depth], right).astype(BF16)
        copy(t).start()
    for t in range(steps):
        copy(t).wait()


def groups_of(shape, dim, size):
    index = iota(shape, dim)
    group = jnp.floor((index.astype(F32) + 0.5) * (1.0 / size)).astype(jnp.int32)
    return group, index - group * size


def target_kernel(ids_ref, after_ref, place_ref):
    devices = ids_ref.shape[0]
    columns, count = place_ref.shape
    by_row = ids_ref[...].astype(F32).T[0:ROWS, :].astype(jnp.int32) + 1
    halves = jnp.concatenate(
        [lax.shift_right_logical(by_row, 5).astype(F32), (by_row & 31).astype(F32)], axis=0
    ).astype(BF16)
    owner, _ = groups_of((devices, count), 1, RANKS)
    both = dot(halves, one_hot(owner == iota((devices, count), 0)))
    both = both[0:ROWS] * 32.0 + both[ROWS:]
    _, rank = groups_of((ROWS, count), 1, RANKS)
    mine = rank == iota((ROWS, count), 0)
    wanted = jnp.sum(jnp.where(mine, both, 0.0), axis=0, keepdims=True).astype(jnp.int32) - 1
    step = 256
    for k in range(0, columns, step):
        place_ref[k : k + step, :] = one_hot(iota((step, count), 0) + k == wanted)


def final_kernel(place_ref, base_ref, back_ref, grad_ref, bias_ref, table, *, scaling):
    columns, count = place_ref.shape
    devices = count // RANKS
    rows = back_ref.shape[0]
    chunk = rows // devices
    npred, share = bias_ref.shape
    _, inside = groups_of((ROWS, rows), 1, chunk)
    last = one_hot(inside == iota((ROWS, rows), 0) + (chunk - BIAS_ROWS))
    total = dot(last, back_ref[...])
    total = jnp.concatenate([total[q : q + 1, :] for q in range(BIAS_ROWS)], axis=1)
    high, low = total[:, 0 : npred * share], total[:, npred * share :]
    spare = npred * share - low.shape[1]
    total = (high + jnp.concatenate([low, jnp.zeros((1, spare), F32)], axis=1)) * scaling
    for p in range(npred):
        bias_ref[p : p + 1, :] = total[:, p * share : (p + 1) * share]
    reorder(back_ref, table, chunk, 1)
    step = 256
    for k in range(0, columns, step):
        jacobian = 1.0 + 0.5 * jnp.tanh(base_ref[k : k + step, :].astype(F32))
        grad = dot(place_ref[k : k + step, :], table[...]) * jacobian
        grad_ref[k : k + step, :] = grad.astype(BF16)


def exchange(x):
    return lax.all_to_all(x, AXES, split_axis=0, concat_axis=0, tiled=True)


def shards(
    background,
    increment,
    coefficients,
    departures,
    bias_pred,
    beta_incr,
    obs_weight,
    obs_count,
    col_index,
):
    devices = lax.axis_size(AXES)
    columns, profile = background.shape
    blocks, block_len = col_index.shape
    channels = coefficients.shape[1]
    npred = bias_pred.shape[2]
    slots = blocks * block_len
    shift = columns.bit_length() - 1
    assert columns == 1 << shift and channels % (TILE * 1) == 0
    scaling = float((slots * devices) ** -0.5)
    depth = profile + 4 * npred
    group = RANKS * profile // LANES
    chunk = group + BIAS_ROWS

    def shape(*dims, dtype=BF16):
        return jax.ShapeDtypeStruct(dims, dtype)

    def call(kernel, outs, inputs, flops, in_specs=None, out_specs=None, scratch=(), vmem=None):
        return pl.pallas_call(
            kernel,
            out_shape=outs,
            in_specs=in_specs or [VMEM] * len(inputs),
            out_specs=out_specs or ([VMEM] * len(outs) if isinstance(outs, tuple) else VMEM),
            scratch_shapes=scratch,
            compiler_params=pltpu.CompilerParams(vmem_limit_bytes=vmem and vmem * 2**20),
            cost_estimate=pl.CostEstimate(
                flops=int(flops), bytes_accessed=4 * 2**20, transcendentals=0
            ),
        )(*inputs)

    def in_hbm(x):
        return pltpu.with_memory_space_constraint(x, pltpu.HBM)

    flat_dep = in_hbm(departures.reshape(slots, channels))
    coef_hbm = in_hbm(coefficients)
    requests, position, formed = call(
        lambda *refs: index_kernel(*refs, shift=shift),
        (
            shape(devices, LANES, dtype=jnp.int32),
            shape(blocks, block_len, dtype=jnp.int32),
            shape(columns, profile),
        ),
        (in_hbm(col_index), in_hbm(background), in_hbm(increment)),
        1e8,
        in_specs=[ANY] * 3,
        scratch=[
            pltpu.VMEM((blocks, block_len), jnp.int32),
            pltpu.VMEM((columns, profile), BF16),
            pltpu.VMEM((columns, profile), BF16),
            pltpu.SemaphoreType.DMA((9,)),
        ],
        vmem=16,
    )
    ids = exchange(requests.reshape(devices, 1, LANES)).reshape(devices, LANES)
    ids, obs_weight = lax.optimization_barrier((ids, obs_weight))
    weight = obs_weight.reshape(1, channels)
    rows_out = call(
        owner_kernel,
        shape(devices * group, LANES),
        (ids, formed),
        1e9,
        out_specs=ANY,
        scratch=[
            pltpu.VMEM((devices * RANKS, columns), BF16),
            pltpu.VMEM((devices * group, LANES), F32),
            pltpu.VMEM((devices * group, LANES), BF16),
            pltpu.SemaphoreType.DMA((2,)),
        ],
        vmem=16,
    )
    arrived = exchange(rows_out.reshape(devices, group // 2, 2, LANES))
    arrived = arrived.reshape(devices * group, LANES)
    slot_pos, norm, base, base_sums, side, stack = call(
        second_kernel,
        (
            shape(blocks, block_len, dtype=jnp.int32),
            shape(depth, 2 * profile),
            shape(slots, profile, dtype=F32),
            shape(npred, channels, dtype=F32),
            shape(slots, LANES),
            shape(2 * npred, slots),
        ),
        (
            ids,
            position,
            jnp.transpose(bias_pred, (0, 2, 1)),
            obs_count,
            beta_incr,
            weight,
            coef_hbm,
            flat_dep,
        ),
        8e9,
        in_specs=[ANY, VMEM, VMEM, SMEM, VMEM, VMEM, ANY, ANY],
        scratch=[
            pltpu.VMEM((profile, channels), BF16),
            pltpu.VMEM((slots, channels), BF16),
            pltpu.VMEM((profile, channels), BF16),
            pltpu.SemaphoreType.DMA((4,)),
            pltpu.SemaphoreType.DMA((4,)),
        ],
        vmem=32,
    )
    outgoing, left = call(
        main_kernel,
        (
            shape(devices * chunk, LANES),
            pltpu.HBM((slots, profile + LANES), BF16),
        ),
        (arrived, slot_pos, side, stack, norm, base, weight, base_sums, beta_incr, coef_hbm),
        2e9,
        in_specs=[VMEM] * 9 + [ANY],
        out_specs=(ANY, ANY),
        scratch=[
            pltpu.VMEM((slots, profile + LANES), BF16),
            pltpu.VMEM((npred, channels), F32),
            pltpu.VMEM((devices, npred, LANES), F32),
            pltpu.VMEM((devices * chunk, LANES), F32),
            pltpu.VMEM((profile, channels), BF16),
            pltpu.VMEM((devices * chunk, LANES), BF16),
            pltpu.VMEM((devices * RANKS, profile), BF16),
            pltpu.VMEM((slots, devices * RANKS), BF16),
            pltpu.SemaphoreType.DMA,
            pltpu.SemaphoreType.DMA((2,)),
            pltpu.SemaphoreType.DMA,
        ],
        vmem=24,
    )
    returned = exchange(outgoing.reshape(devices, chunk // 2, 2, LANES))
    returned = returned.reshape(devices * chunk, LANES)
    place = call(
        target_kernel,
        shape(columns, devices * RANKS),
        (ids, in_hbm(left)),
        1e9,
        in_specs=[VMEM, ANY],
        vmem=16,
    )
    radiance = call(
        radiance_kernel,
        shape(slots, channels),
        (left, beta_incr, coef_hbm),
        3e9,
        in_specs=[VMEM, VMEM, ANY],
        out_specs=ANY,
        scratch=[
            pltpu.VMEM((slots, channels), BF16),
            pltpu.VMEM((profile, channels), BF16),
            pltpu.SemaphoreType.DMA((channels // TILE,)),
            pltpu.SemaphoreType.DMA,
        ],
        vmem=32,
    )
    column_grad, bias_grad = call(
        lambda *refs: final_kernel(*refs, scaling=scaling),
        (shape(columns, profile), shape(npred, channels // devices, dtype=F32)),
        (place, background, returned),
        1e9,
        scratch=[pltpu.VMEM((devices * RANKS, profile), BF16)],
        vmem=16,
    )
    return (
        radiance.reshape(blocks, block_len, channels),
        column_grad,
        jnp.transpose(bias_grad, (1, 0)),
    )


def solution(mesh):
    finer = Mesh(mesh.devices.reshape(4, 2, 4, 4), AXES)
    in_specs = (
        P(AXES, None),
        P(AXES, None),
        P(),
        P(AXES, None, None),
        P(AXES, None, None),
        P(),
        P(),
        P(AXES),
        P(AXES, None),
    )
    out_specs = (P(AXES, None, None), P(AXES, None), P(AXES, None))
    return jax.shard_map(
        shards, mesh=finer, in_specs=in_specs, out_specs=out_specs, check_vma=False
    )
```
